256 devices in a mesh: group: 16 (over z, core), dp: 16 (over x, y).
Axes of the slice: x: 4, y: 4, z: 8, core: 2. Of those that a mesh axis runs over, the one named last changes fastest.
Arguments:
- resp_q: bfloat16 [16, 4096, 4096], P('group', 'dp'), may hold values from -410 to 410
- resp_k: bfloat16 [16, 4096, 4096], P('group', 'dp'), may hold values from -410 to 410
- resp_v: bfloat16 [16, 4096, 4096], P('group', 'dp'), may hold values from -6 to 6
- prompt_k: bfloat16 [16, 2048, 4096], P('group', 'dp'), may hold values from -410 to 410
- prompt_v: bfloat16 [16, 2048, 4096], P('group', 'dp'), may hold values from -6 to 6
- prompt_len: int32 [16], P('group'), may hold values from 512 to 2048
- resp_len: int32 [16, 16], P('group', 'dp'), may hold values from 1 to 256, as said below
- assign: int32 [16, 32], P('group', 'dp'), may hold values from 0 to 63, as said below
- rewards: float32 [16, 16], P('group', 'dp'), may hold values from -18 to 18
- feat_q: bfloat16 [32, 128, 128], replicated, may hold values from -1 to 1
- feat_k: bfloat16 [32, 128, 128], replicated, may hold values from -1 to 1
Outputs:
- attn_out: bfloat16 [16, 2048, 4096], P('group', 'dp')
- token_adv: float32 [16, 2048], P('group', 'dp')
The draws below stay inside these ranges and needn't reach their ends.
Inputs may be any that keep to these rules, and one draw needn't show every extreme that they name: Response r of a prompt has ceil(resp_len / 64) live blocks; these counts sum to 2 * 16 over a prompt's responses, and one response of every prompt has 4 blocks. `assign`: entry d * 2 + j names the block r * 4 + c (block c of response r) whose outputs go to slot j of device d of dp. Every live block of the prompt is named exactly once, and the 2 slots of one device name blocks of different responses.
All inputs are finite; a program needn't handle non-finite values.
Results may differ from the reference program's by a relative error of at most 0.0085.
Values may be sent and summed in bfloat16 or wider, within the bound.
No kernel may reach another device: no remote copies, remote signals or barrier semaphores. Data moves between devices by JAX's collectives and lax.ppermute only.
A program may use at most 128 MiB of HBM per device.

```python
import jax
import jax.numpy as jnp
from jax import lax

H = 32
DH = 128
FH = 128
BLK = 64
MAXC = 4
CAP = 2
PT_DEV = 128
PROMPTS = 16
RESP = 16


def heavy_draw(key, rows, salt):
    stream = jax.random.fold_in(key, salt)
    first_key = jax.random.fold_in(stream, 0)
    extent = (PROMPTS, rows, H * DH)
    sample = jnp.clip(jax.random.normal(first_key, extent, jnp.float32), -6.0, 6.0)
    return sample.astype(jnp.bfloat16)


def draw_resp_q(key, part):
    return heavy_draw(key, RESP * MAXC * BLK, 101)


def draw_resp_k(key, part):
    return heavy_draw(key, RESP * MAXC * BLK, 202)


def draw_prompt_k(key, part):
    return heavy_draw(key, RESP * PT_DEV, 303)


def draw_rewards(key, part):
    stream = jax.random.fold_in(key, 404)
    first_key = jax.random.fold_in(stream, 0)
    rising = 1.0 + 2.0 * jnp.arange(PROMPTS, dtype=jnp.float32)[:, None] / (PROMPTS - 1)
    sample = jnp.clip(jax.random.normal(first_key, (PROMPTS, RESP), jnp.float32), -6.0, 6.0) * rising
    return sample


def stretch_plan(key):

    def per_prompt(prompt_key):
        slot_key, lead_key, tail_key, order_key, device_key = jax.random.split(prompt_key, 5)
        slots = RESP * (MAXC - 1)
        counter = jnp.arange(slots, dtype=jnp.int32)
        ranking = jax.random.randint(slot_key, (slots,), 0, 1 << 20).astype(jnp.int32) * slots + counter
        leader = jax.random.randint(lead_key, (), 0, RESP).astype(jnp.int32)
        owner = counter // (MAXC - 1)
        ranking = jnp.where(owner == leader, (1 << 20) * slots + counter, ranking)
        ordering = jnp.argsort(-ranking)
        chosen = jnp.zeros((slots,), jnp.int32).at[ordering[:RESP * (CAP - 1)]].set(1)
        blocks = 1 + chosen.reshape(RESP, MAXC - 1).sum(axis=1)
        tails = jax.random.randint(tail_key, (RESP,), 1, BLK + 1).astype(jnp.int32)
        tokens = (blocks - 1) * BLK + tails
        index_row = jnp.arange(RESP, dtype=jnp.int32)
        sigma = jnp.argsort(jax.random.randint(order_key, (RESP,), 0, 1 << 20).astype(jnp.int32) * RESP + index_row)
        devperm = jnp.argsort(jax.random.randint(device_key, (RESP,), 0, 1 << 20).astype(jnp.int32) * RESP + index_row)
        ordered = blocks[sigma]
        starts = jnp.cumsum(ordered) - ordered
        stream_index = jnp.arange(RESP * CAP, dtype=jnp.int32)
        located = jnp.sum((starts[None, :] <= stream_index[:, None]).astype(jnp.int32), axis=1) - 1
        response = sigma[located]
        within = stream_index - starts[located]
        target = devperm[stream_index % RESP] * CAP + stream_index // RESP
        table = jnp.zeros((RESP * CAP,), jnp.int32).at[target].set((response * MAXC + within).astype(jnp.int32))
        return (tokens.astype(jnp.int32), table)
    prompt_keys = jax.random.split(jax.random.fold_in(key, 505), PROMPTS)
    return jax.vmap(per_prompt)(prompt_keys)


def draw_resp_len(key, part):
    return stretch_plan(key)[0]


def draw_assign(key, part):
    return stretch_plan(key)[1]


def set_ends(result, stream_key, least, top_value):
    longest = result.shape.index(max(result.shape))
    spots = []
    for shift in (0, 1):
        where = [jax.random.randint(jax.random.fold_in(stream_key, axis), (), 0, length) for axis, length in enumerate(result.shape)]
        where[longest] = (where[longest] + shift) % result.shape[longest]
        spots.append(tuple(where))
    return result.at[spots[0]].set(least).at[spots[1]].set(top_value)


def steps_of(own_key, shape, shards, least, largest):
    def one(position, parts):
        heights = jax.random.uniform(jax.random.fold_in(jax.random.fold_in(own_key, 6), position), (parts,), jnp.float32, least / len(shards), largest / len(shards))
        return jnp.repeat(jnp.exp(heights), shape[position] // parts).reshape((-1,) + (1,) * (len(shape) - position - 1))

    level = one(*shards[0])
    for cut in shards[1:]:
        level = level * one(*cut)
    return level


def bell_draw(stream_key, dims, scale, reach, cuts=(), held_as=jnp.bfloat16):
    array = scale * jax.random.normal(stream_key, dims, jnp.float32)
    if cuts:
        array = array * steps_of(stream_key, dims, cuts, -0.22, 0.18)
    return jnp.clip(array, -reach, reach).astype(held_as)


def setup_inputs(seed: int = 0) -> dict:
    splits = jax.random.split(jax.random.key(seed), 12)
    resp_q = draw_resp_q(jax.random.fold_in(splits[11], 71), 0)
    resp_k = draw_resp_k(jax.random.fold_in(splits[11], 71), 0)
    resp_v = bell_draw(splits[2], (PROMPTS, RESP * MAXC * BLK, H * DH), 1.0, 6.0, ((0, 16), (1, 16)))
    prompt_k = draw_prompt_k(jax.random.fold_in(splits[11], 71), 0)
    prompt_v = bell_draw(splits[4], (PROMPTS, RESP * PT_DEV, H * DH), 1.0, 6.0, ((0, 16), (1, 16)))
    prompt_len = set_ends(jax.random.randint(splits[5], (PROMPTS,), RESP * PT_DEV // 4, RESP * PT_DEV + 1), jax.random.fold_in(splits[5], 1), RESP * PT_DEV // 4, RESP * PT_DEV).astype(jnp.int32)
    resp_len = draw_resp_len(jax.random.fold_in(splits[11], 71), 0)
    assign = draw_assign(jax.random.fold_in(splits[11], 71), 0)
    rewards = draw_rewards(jax.random.fold_in(splits[11], 71), 0)
    feat_q = bell_draw(splits[9], (H, DH, FH), (DH // 4) ** -0.5, 1.0)
    feat_k = bell_draw(splits[10], (H, DH, FH), (DH // 4) ** -0.5, 1.0)
    return dict(resp_q=resp_q, resp_k=resp_k, resp_v=resp_v, prompt_k=prompt_k, prompt_v=prompt_v, prompt_len=prompt_len, resp_len=resp_len, assign=assign, rewards=rewards, feat_q=feat_q, feat_k=feat_k)


def features(rows, weights):
    logits = jnp.einsum('thd,hdf->thf', rows.astype(jnp.float32), weights.astype(jnp.float32), precision=lax.Precision.HIGHEST)
    return jnp.concatenate([jax.nn.softmax(logits, axis=-1), jax.nn.softmax(-logits, axis=-1)], axis=-1).astype(jnp.bfloat16)

def reference(resp_q, resp_k, resp_v, prompt_k, prompt_v, prompt_len, resp_len, assign, rewards, feat_q, feat_k):
    head_count = feat_q.shape[0]
    head_width = feat_q.shape[1]
    length = MAXC * BLK
    prompt_rows = prompt_k.shape[1]
    causal = jnp.arange(length)[:, None] >= jnp.arange(length)[None, :]
    highest = lax.Precision.HIGHEST

    def per_prompt(operands):
        queries, key_rows, value_rows, prompt_keys, prompt_values, limit, lengths, slot_ids = operands
        prompt_feat = features(prompt_keys.reshape(prompt_rows, head_count, head_width), feat_k)
        keep = jnp.arange(prompt_rows) < limit
        masked = jnp.where(keep[:, None, None], prompt_feat.astype(jnp.float32), jnp.float32(0.0))
        kv_state = jnp.einsum('shf,she->hfe', masked, prompt_values.reshape(prompt_rows, head_count, head_width).astype(jnp.float32), precision=highest).astype(jnp.bfloat16)
        key_total = lax.optimization_barrier(jnp.sum(masked, axis=0)).astype(jnp.bfloat16)

        def per_response(items):
            query_rows, key_block, value_block, size = items
            query_feat = features(query_rows.reshape(length, head_count, head_width), feat_q).astype(jnp.float32)
            key_feat = features(key_block.reshape(length, head_count, head_width), feat_k).astype(jnp.float32)
            prompt_num = jnp.einsum('thf,hfe->the', query_feat, kv_state.astype(jnp.float32), precision=highest).astype(jnp.bfloat16)
            prompt_den = jnp.einsum('thf,hf->th', query_feat, key_total.astype(jnp.float32), precision=highest).astype(jnp.bfloat16)
            scores = jnp.einsum('thf,shf->hts', query_feat, key_feat, precision=highest)
            scores = jnp.where(causal[None], scores, jnp.float32(0.0))
            intra_den = lax.optimization_barrier(jnp.sum(scores, axis=-1))
            rounded = lax.optimization_barrier(scores.astype(jnp.bfloat16)).astype(jnp.float32)
            values_f = value_block.reshape(length, head_count, head_width).astype(jnp.float32)
            intra_num = jnp.einsum('hts,she->the', rounded, values_f, precision=highest)
            combined = (prompt_num.astype(jnp.float32) + intra_num) / (prompt_den.astype(jnp.float32) + intra_den.T)[:, :, None]
            live_rows = jnp.arange(length) < size
            combined = jnp.where(live_rows[:, None, None], combined, jnp.float32(0.0))
            return combined.astype(jnp.bfloat16).reshape(MAXC, BLK, head_count * head_width)
        outputs = lax.map(per_response, (queries.reshape(RESP, length, head_count * head_width), key_rows.reshape(RESP, length, head_count * head_width), value_rows.reshape(RESP, length, head_count * head_width), lengths))
        flat = outputs.reshape(RESP * MAXC, BLK, head_count * head_width)
        return jnp.take(flat, slot_ids.astype(jnp.int32), axis=0).reshape(RESP * CAP * BLK, head_count * head_width)
    attended = lax.map(per_prompt, (resp_q, resp_k, resp_v, prompt_k, prompt_v, prompt_len, resp_len, assign))
    centred = rewards - lax.optimization_barrier(jnp.mean(rewards, axis=1, keepdims=True))
    spread = jnp.mean(centred * centred)
    advantage = centred / jnp.sqrt(spread + 1e-06)
    responses = (assign // MAXC).astype(jnp.int32)
    pieces = (assign % MAXC).astype(jnp.int32)
    slot_adv = jnp.take_along_axis(advantage, responses, axis=1)
    slot_len = jnp.take_along_axis(resp_len, responses, axis=1)
    positions = pieces[:, :, None] * BLK + jnp.arange(BLK, dtype=jnp.int32)[None, None, :]
    token_adv = jnp.where(positions < slot_len[:, :, None], slot_adv[:, :, None], jnp.float32(0.0))
    return (attended, token_adv.reshape(rewards.shape[0], RESP * CAP * BLK))
```

```python
import jax
import jax.numpy as jnp
from jax import lax
from jax.experimental import pallas as pl
from jax.experimental.pallas import tpu as pltpu
from jax.sharding import PartitionSpec as P

BLK = 64
F32 = jnp.float32
BF16 = jnp.bfloat16
NT = (((1,), (1,)), ((), ()))
TN = (((0,), (0,)), ((), ()))
NN = (((1,), (0,)), ((), ()))


def mm(a, b, dims=NN):
    return lax.dot_general(a, b, dims, preferred_element_type=F32)


def feats(x, w):
    u = mm(x, w)
    ep = jnp.exp(u - jnp.max(u, axis=-1, keepdims=True))
    en = jnp.exp(jnp.min(u, axis=-1, keepdims=True) - u)
    rp = 1.0 / jnp.sum(ep, axis=-1, keepdims=True)
    rn = 1.0 / jnp.sum(en, axis=-1, keepdims=True)
    return jnp.concatenate([ep * rp, en * rn], axis=-1)


def state_kernel(n_ref, k_ref, v_ref, w_ref, o_ref):
    rows, width = k_ref.shape[0], w_ref.shape[1]
    full = 2 * w_ref.shape[2]
    keep = lax.broadcasted_iota(jnp.int32, (rows, 1), 0) < n_ref[0]
    rid = lax.broadcasted_iota(jnp.int32, (16, rows), 0)
    tot = jnp.zeros((16, full // 2), F32)
    for h in range(2):
        cols = slice(h * width, (h + 1) * width)
        phi = jnp.where(keep, feats(k_ref[:, cols], w_ref[h]), 0.0).astype(BF16)
        o_ref[0, h * full : (h + 1) * full, :] = mm(phi, v_ref[:, cols], TN).astype(BF16)
        for s in range(2):
            pick = (rid == 2 * h + s).astype(BF16)
            tot = tot + mm(pick, phi[:, s * full // 2 : (s + 1) * full // 2])
    o_ref[0, 2 * full : 2 * full + 16, :] = tot.astype(BF16)


def intra_kernel(q_ref, k_ref, v_ref, wq_ref, wk_ref, o_ref):
    length = q_ref.shape[0]
    pieces = length // BLK
    pq = feats(q_ref[...], wq_ref[0]).astype(BF16)
    pk = feats(k_ref[...], wk_ref[0]).astype(BF16)
    score = mm(pq, pk, NT)
    t = lax.broadcasted_iota(jnp.int32, score.shape, 0)
    s = lax.broadcasted_iota(jnp.int32, score.shape, 1)
    score = jnp.where(s <= t, score, 0.0)
    hi = score.astype(BF16)
    lo = (score - hi.astype(F32)).astype(BF16)
    o_ref[0, :length, :] = mm(hi, v_ref[...]).astype(BF16)
    rid = lax.broadcasted_iota(jnp.int32, (16, length), 0)
    den = jnp.zeros((16, BLK), F32)
    for c in range(pieces):
        pick = (rid // 2 == c).astype(BF16)
        rows = slice(c * BLK, (c + 1) * BLK)
        den = den + mm(pick, hi[rows], NT) + mm(pick, lo[rows], NT)
    dhi = den.astype(BF16).astype(F32)
    odd = lax.broadcasted_iota(jnp.int32, den.shape, 0) % 2 == 1
    den = jnp.where(odd, den - dhi, dhi).astype(BF16)
    o_ref[0, length:, :] = jnp.concatenate([den, jnp.zeros_like(den)], axis=1)


def prompt_kernel(ids_ref, q_ref, part_ref, w_ref, num_ref, den_ref, s_ref, t_ref):
    i = pl.program_id(0)
    width = w_ref.shape[1]
    full = 2 * w_ref.shape[2]
    many = num_ref.shape[1]

    @pl.when(i == 0)
    def _():
        acc = part_ref[0].astype(F32)
        for d in range(1, part_ref.shape[0]):
            acc = acc + part_ref[d].astype(F32)
        acc = acc.astype(BF16)
        s_ref[...] = acc[: 2 * full]
        tail = acc[2 * full :].astype(F32)
        for h in range(2):
            row = jnp.concatenate([tail[2 * h : 2 * h + 1], tail[2 * h + 1 : 2 * h + 2]], axis=1)
            t_ref[h] = jnp.broadcast_to(row, t_ref.shape[1:]).astype(BF16)

    rows = []
    for j in range(many):
        b = ids_ref[i * many + j]
        pieces = q_ref.shape[1] // BLK
        rows.append(q_ref[b // pieces, pl.ds(pl.multiple_of(b % pieces * BLK, BLK), BLK), :])
    x = jnp.concatenate(rows, axis=0)
    for h in range(2):
        phi = feats(x[:, h * width : (h + 1) * width], w_ref[h]).astype(BF16)
        num = mm(phi, s_ref[h * full : (h + 1) * full, :]).astype(BF16)
        den = mm(phi, t_ref[h], NT).astype(BF16)
        num_ref[h] = num.reshape(many, BLK, width)
        den_ref[h] = den.reshape(many, BLK, width)


def combine_kernel(ids_ref, len_ref, part_ref, num_ref, den_ref, o_ref):
    length = part_ref.shape[1] - 16
    pieces = length // BLK
    many = num_ref.shape[1]
    rid = lax.broadcasted_iota(jnp.int32, (16, part_ref.shape[2]), 0)
    row = lax.broadcasted_iota(jnp.int32, (BLK, 1), 0)
    for j in range(many):
        b = ids_ref[j]
        r, c = b // pieces, b % pieces
        num = part_ref[r, pl.ds(pl.multiple_of(c * BLK, BLK), BLK), :].astype(F32)
        pick = (rid // 2 == c).astype(BF16)
        den = mm(part_ref[r, length:, :BLK], pick, TN)
        num = num_ref[0, j].astype(F32) + num
        den = den_ref[0, j].astype(F32) + den
        out = jnp.where(row < len_ref[r] - c * BLK, num / den, 0.0)
        o_ref[j * BLK : (j + 1) * BLK, :] = out.astype(BF16)


def place_kernel(a_ref, b_ref, o_ref):
    width = a_ref.shape[2]
    for o in range(a_ref.shape[0]):
        o_ref[:, 2 * o * width : (2 * o + 1) * width] = a_ref[o]
        o_ref[:, (2 * o + 1) * width : (2 * o + 2) * width] = b_ref[o]


def body(
    resp_q,
    resp_k,
    resp_v,
    prompt_k,
    prompt_v,
    prompt_len,
    resp_len,
    assign,
    rewards,
    feat_q,
    feat_k,
):
    dp = lax.axis_size("dp")
    groups = lax.axis_size("group")
    me = lax.axis_index("dp")
    heads, width, feat = feat_q.shape
    length = resp_q.shape[1]
    pieces = length // BLK
    prompt_rows = prompt_k.shape[1]
    slots = assign.shape[1]
    two = 2 * width
    q, k, v, pk, pv = resp_q[0], resp_k[0], resp_v[0], prompt_k[0], prompt_v[0]

    tiny = jnp.concatenate(
        [assign[0].astype(F32), resp_len[0].astype(F32), rewards[0]]
    )
    tiny = lax.all_to_all(
        jnp.broadcast_to(tiny[None], (dp, slots + 2)), "dp", 0, 0, tiled=True
    )
    ids = tiny[:, :slots].astype(jnp.int32).reshape(-1)
    lens = tiny[:, slots].astype(jnp.int32)
    reward_all = tiny[:, slots + 1]

    q_all = lax.all_to_all(q, "dp", split_axis=1, concat_axis=0, tiled=True).reshape(
        dp, length, two
    )

    keep = jnp.clip(prompt_len[0] - me * prompt_rows, 0, prompt_rows).astype(jnp.int32)
    state_rows = 4 * feat + 16
    part = pl.pallas_call(
        state_kernel,
        grid=(dp,),
        in_specs=[
            pl.BlockSpec(memory_space=pltpu.SMEM),
            pl.BlockSpec((prompt_rows, two), lambda o: (0, o)),
            pl.BlockSpec((prompt_rows, two), lambda o: (0, o)),
            pl.BlockSpec((2, width, feat), lambda o: (o, 0, 0)),
        ],
        out_specs=pl.BlockSpec((1, state_rows, width), lambda o: (o, 0, 0)),
        out_shape=jax.ShapeDtypeStruct((dp, state_rows, width), BF16),
        name="state",
    )(keep.reshape(1), pk, pv, feat_k)
    part = lax.all_to_all(part, "dp", 0, 0, tiled=True)

    inner = []
    for p in range(2):
        piece = pl.pallas_call(
            intra_kernel,
            grid=(dp,),
            in_specs=[
                pl.BlockSpec((length, width), lambda o, p=p: (0, 2 * o + p)),
                pl.BlockSpec((length, width), lambda o, p=p: (0, 2 * o + p)),
                pl.BlockSpec((length, width), lambda o, p=p: (0, 2 * o + p)),
                pl.BlockSpec((1, width, feat), lambda o, p=p: (2 * o + p, 0, 0)),
                pl.BlockSpec((1, width, feat), lambda o, p=p: (2 * o + p, 0, 0)),
            ],
            out_specs=pl.BlockSpec((1, length + 16, width), lambda o: (o, 0, 0)),
            out_shape=jax.ShapeDtypeStruct((dp, length + 16, width), BF16),
            name="intra",
        )(q, k, v, feat_q, feat_k)
        inner.append(lax.all_to_all(piece, "dp", 0, 0, tiled=True))

    total = dp * slots
    many = 4
    own_w = lax.dynamic_slice_in_dim(feat_q, 2 * me, 2, 0)
    num, den = pl.pallas_call(
        prompt_kernel,
        grid=(total // many,),
        in_specs=[
            pl.BlockSpec(memory_space=pltpu.SMEM),
            pl.BlockSpec((dp, length, two), lambda i: (0, 0, 0)),
            pl.BlockSpec((dp, state_rows, width), lambda i: (0, 0, 0)),
            pl.BlockSpec((2, width, feat), lambda i: (0, 0, 0)),
        ],
        out_specs=[
            pl.BlockSpec((2, many, BLK, width), lambda i: (0, i, 0, 0)),
            pl.BlockSpec((2, many, BLK, width), lambda i: (0, i, 0, 0)),
        ],
        out_shape=[
            jax.ShapeDtypeStruct((2, total, BLK, width), BF16),
            jax.ShapeDtypeStruct((2, total, BLK, width), BF16),
        ],
        scratch_shapes=[
            pltpu.VMEM((4 * feat, width), BF16),
            pltpu.VMEM((2, width, 2 * feat), BF16),
        ],
        name="prompt",
    )(ids, q_all, part, own_w)

    outs = []
    for p in range(2):
        piece = pl.pallas_call(
            combine_kernel,
            in_specs=[
                pl.BlockSpec(memory_space=pltpu.SMEM),
                pl.BlockSpec(memory_space=pltpu.SMEM),
                pl.BlockSpec((dp, length + 16, width), lambda i: (0, 0, 0)),
                pl.BlockSpec((1, total, BLK, width), lambda i, p=p: (p, 0, 0, 0)),
                pl.BlockSpec((1, total, BLK, width), lambda i, p=p: (p, 0, 0, 0)),
            ],
            grid=(1,),
            out_specs=pl.BlockSpec((total * BLK, width), lambda i: (0, 0)),
            out_shape=jax.ShapeDtypeStruct((total * BLK, width), BF16),
            name="combine",
        )(ids, lens, inner[p], num, den)
        outs.append(
            lax.all_to_all(piece.reshape(dp, slots * BLK, width), "dp", 0, 0, tiled=True)
        )
    attn = pl.pallas_call(
        place_kernel,
        out_shape=jax.ShapeDtypeStruct((slots * BLK, heads * width), BF16),
        name="place",
    )(*outs)

    centred = reward_all - jnp.sum(reward_all) / dp
    squares = jnp.sum(centred * centred)
    spread = jnp.sum(
        lax.all_to_all(jnp.broadcast_to(squares, (groups, 1)), "group", 0, 0, tiled=True)
    )
    advantage = centred / jnp.sqrt(spread / (groups * dp) + 1e-06)
    own = assign[0]
    picker = (own // pieces)[:, None] == jnp.arange(dp)[None, :]
    slot_adv = jnp.sum(jnp.where(picker, advantage[None, :], 0.0), axis=1)
    slot_len = jnp.sum(jnp.where(picker, lens[None, :], 0), axis=1)
    positions = (own % pieces)[:, None] * BLK + jnp.arange(BLK)[None, :]
    token_adv = jnp.where(positions < slot_len[:, None], slot_adv[:, None], F32(0.0))
    return (attn[None], token_adv.reshape(1, slots * BLK))


def solution(mesh):
    return jax.shard_map(
        body,
        mesh=mesh,
        in_specs=(
            P("group", "dp", None),
            P("group", "dp", None),
            P("group", "dp", None),
            P("group", "dp", None),
            P("group", "dp", None),
            P("group"),
            P("group", "dp"),
            P("group", "dp"),
            P("group", "dp"),
            P(),
            P(),
        ),
        out_specs=(P("group", "dp", None), P("group", "dp")),
        check_vma=False,
    )
```

```python
import jax
import jax.numpy as jnp
from jax import lax
from jax.experimental import pallas as pl
from jax.experimental.pallas import tpu as pltpu
from jax.sharding import PartitionSpec as P


BLK = 64
SIDE = 4
EXTRA = 8
F32 = jnp.float32
BF16 = jnp.bfloat16
NT = (((1,), (1,)), ((), ()))
TN = (((0,), (0,)), ((), ()))
NN = (((1,), (0,)), ((), ()))


def mm(a, b, dims=NN):
    return lax.dot_general(a, b, dims, preferred_element_type=F32)


def feats(x, w):
    u = mm(w.T, x, NT)
    ep = jnp.exp(u - jnp.max(u, axis=0, keepdims=True))
    en = jnp.exp(jnp.min(u, axis=0, keepdims=True) - u)
    rp = 1.0 / jnp.sum(ep, axis=0, keepdims=True)
    rn = 1.0 / jnp.sum(en, axis=0, keepdims=True)
    return jnp.concatenate([ep * rp, en * rn], axis=0)


def spread_kernel(tab_ref, q_ref, o_ref):
    length, width = q_ref.shape[0], o_ref.shape[2]
    part = width // 8
    r = jnp.broadcast_to(tab_ref[...], (EXTRA, width))
    col = lax.broadcasted_iota(jnp.int32, r.shape, 1)
    r1 = r.astype(BF16).astype(F32)
    r2 = (r - r1).astype(BF16).astype(F32)
    r3 = r - r1 - r2
    tabs = jnp.where(col < 2 * part, r1, jnp.where(col < 3 * part, r2, r3)).astype(BF16)
    for o in range(o_ref.shape[0]):
        o_ref[o, :length, :] = q_ref[:, o * width : (o + 1) * width]
        o_ref[o, length:, :] = tabs


def state_kernel(at_ref, *refs):
    ins, outs = refs[:6], refs[6:]
    rows, width = ins[0].shape
    keep = lax.broadcasted_iota(jnp.int32, (1, rows), 1) < at_ref[2]
    rid = lax.broadcasted_iota(jnp.int32, (EXTRA, rows), 0)
    shift = pl.program_id(0)
    for p in range(2):
        k_ref, v_ref, w_ref = ins[3 * p : 3 * p + 3]
        phi = jnp.where(keep, feats(k_ref[...], w_ref[0]), 0.0).astype(BF16)
        half = phi.shape[0] // 2
        state = mm(phi, v_ref[...]).astype(BF16)
        tail = jnp.zeros((EXTRA, width), F32)
        for i in range(2):
            pick = (rid == i).astype(BF16)
            tail = tail + mm(pick, phi[i * half : (i + 1) * half], NT)
        tail = tail.astype(BF16)
        for s in range(SIDE):

            @pl.when(shift == s)
            def _(o_ref=outs[SIDE * p + s], state=state, tail=tail):
                o_ref[0, : 2 * half, :] = state
                o_ref[0, 2 * half :, :] = tail


def add_kernel(at_ref, *refs):
    ins, outs = refs[: 2 * SIDE], refs[2 * SIDE :]
    for p in range(2):
        for s in range(SIDE):
            j = (at_ref[1 - p] + s) % SIDE
            acc = ins[SIDE * p][j].astype(F32)
            for i in range(1, SIDE):
                acc = acc + ins[SIDE * p + i][j].astype(F32)
            outs[SIDE * p + s][...] = acc.astype(BF16)


def intra_kernel(q_ref, k_ref, v_ref, wq_ref, wk_ref, *rest):
    o_ref = rest[-1]
    length = q_ref.shape[0]
    half = length // 2
    pq = feats(q_ref[...], wq_ref[0]).astype(BF16).T
    pk = feats(k_ref[...], wk_ref[0]).astype(BF16)
    score = mm(pq, pk)
    t = lax.broadcasted_iota(jnp.int32, score.shape, 0)
    s = lax.broadcasted_iota(jnp.int32, score.shape, 1)
    score = jnp.where(s <= t, score, 0.0)
    o_ref[0, :length, :] = mm(score.astype(BF16), v_ref[...]).astype(BF16)
    fold = score[:, :half] + score[:, half:]
    hi = fold.astype(BF16)
    lo = (fold - hi.astype(F32)).astype(BF16)
    ones = jnp.ones((EXTRA, length), BF16)
    den = mm(ones, jnp.concatenate([hi, lo], axis=1), NT)
    rid = lax.broadcasted_iota(jnp.int32, (EXTRA, half), 0)
    den = jnp.where(rid < 2, den[:, :half], den[:, half:])
    dhi = den.astype(BF16).astype(F32)
    den = jnp.where(rid % 2 == 1, den - dhi, dhi)
    o_ref[0, length:, :] = den.astype(BF16)


def prompt_kernel(ids_ref, q_ref, w_ref, *refs):
    parts = refs[: 2 * SIDE]
    num_ref, den_ref, s_ref, t_ref = refs[2 * SIDE :]
    i = pl.program_id(0)
    width = w_ref.shape[1]
    full = 2 * w_ref.shape[2]
    many = num_ref.shape[0]

    @pl.when(i == 0)
    def _():
        for h in range(2):
            acc = parts[SIDE * h][...].astype(F32)
            for d in range(1, SIDE):
                acc = acc + parts[SIDE * h + d][...].astype(F32)
            s_ref[h] = acc[:full].astype(BF16)
            row = jnp.concatenate([acc[full : full + 1], acc[full + 1 : full + 2]], axis=1)
            t_ref[h] = jnp.broadcast_to(row, t_ref.shape[1:]).astype(BF16)

    rows = []
    pieces = q_ref.shape[1] // BLK
    for j in range(many):
        b = ids_ref[i * many + j]
        rows.append(q_ref[b // pieces, pl.ds(pl.multiple_of(b % pieces * BLK, BLK), BLK), :])
    x = jnp.concatenate(rows, axis=0)
    for h in range(2):
        cols = slice(h * width, (h + 1) * width)
        phi = feats(x[:, cols], w_ref[h]).astype(BF16).T
        num = mm(phi, s_ref[h]).astype(BF16)
        den = mm(phi, t_ref[h], NT).astype(BF16)
        num_ref[:, :, cols] = num.reshape(many, BLK, width)
        den_ref[:, :, cols] = den.reshape(many, BLK, width)


def combine_kernel(ids_ref, len_ref, part_ref, num_ref, den_ref, o_ref):
    length = part_ref.shape[1] - EXTRA
    width = part_ref.shape[2] // 2
    pieces = length // BLK
    many = num_ref.shape[0]
    i = pl.program_id(0)
    rid = lax.broadcasted_iota(jnp.int32, (EXTRA, width), 0)
    row = lax.broadcasted_iota(jnp.int32, (BLK, 1), 0)
    for j in range(many):
        b = ids_ref[i * many + j]
        r, c = b // pieces, b % pieces
        pick = (rid // 2 == c // 2).astype(BF16)
        for h in range(2):
            cols = slice(h * width, (h + 1) * width)
            num = part_ref[r, pl.ds(pl.multiple_of(c * BLK, BLK), BLK), cols].astype(F32)
            den = mm(part_ref[r, length:, cols], pick, TN)
            den = jnp.where(c % 2 == 0, den[:BLK], den[BLK:])
            num = num_ref[j, :, cols].astype(F32) + num
            den = den_ref[j, :, cols].astype(F32) + den
            out = jnp.where(row < len_ref[r] - c * BLK, num / den, 0.0)
            o_ref[j * BLK : (j + 1) * BLK, cols] = out.astype(BF16)


def place_kernel(a_ref, o_ref):
    width = a_ref.shape[2]
    for o in range(a_ref.shape[0]):
        o_ref[:, o * width : (o + 1) * width] = a_ref[o]


def hop(dx, dy):
    return [
        (x * SIDE + y, (x + dx) % SIDE * SIDE + (y + dy) % SIDE)
        for x in range(SIDE)
        for y in range(SIDE)
    ]


def body(
    resp_q,
    resp_k,
    resp_v,
    prompt_k,
    prompt_v,
    prompt_len,
    resp_len,
    assign,
    rewards,
    feat_q,
    feat_k,
):
    dp = lax.axis_size("dp")
    groups = lax.axis_size("group")
    me = lax.axis_index("dp")
    heads, width, feat = feat_q.shape
    length = resp_q.shape[1]
    pieces = length // BLK
    prompt_rows = prompt_k.shape[1]
    slots = assign.shape[1]
    two = 2 * width
    tall = length + EXTRA
    q, k, v, pk, pv = resp_q[0], resp_k[0], resp_v[0], prompt_k[0], prompt_v[0]

    part = two // 8
    table = jnp.concatenate(
        [
            assign[0].astype(F32),
            resp_len[0].astype(F32),
            jnp.zeros((part - slots - 1,), F32),
            jnp.broadcast_to(rewards[0], (two - part,)),
        ]
    ).reshape(1, two)
    q_all = pl.pallas_call(
        spread_kernel,
        grid=(4,),
        in_specs=[
            pl.BlockSpec((1, two), lambda o: (0, 0)),
            pl.BlockSpec((length, heads * width // 4), lambda o: (0, o)),
        ],
        out_specs=pl.BlockSpec((dp // 4, tall, two), lambda o: (o, 0, 0)),
        out_shape=jax.ShapeDtypeStruct((dp, tall, two), BF16),
        name="spread",
    )(table, q)
    q_all = lax.all_to_all(q_all, "dp", 0, 0, tiled=True)
    tabs = q_all[:, length, :].astype(F32)
    ids = tabs[:, :slots].astype(jnp.int32).reshape(-1)
    lens = tabs[:, slots].astype(jnp.int32)
    reward_all = tabs[:, part] + tabs[:, 2 * part] + tabs[:, 3 * part]

    keep = jnp.clip(prompt_len[0] - me * prompt_rows, 0, prompt_rows)
    at = jnp.stack([me // SIDE, me % SIDE, keep]).astype(jnp.int32)

    def head(p, s, j, at_ref):
        if p == 0:
            return 2 * ((at_ref[0] + s) % SIDE * SIDE + j)
        return 2 * (j * SIDE + (at_ref[1] + s) % SIDE) + 1

    srows = 2 * feat + EXTRA
    in_specs, out_specs = [], []
    for p in range(2):
        for _ in range(2):
            in_specs.append(
                pl.BlockSpec((prompt_rows, width), lambda s, j, a, p=p: (0, head(p, s, j, a)))
            )
        in_specs.append(
            pl.BlockSpec((1, width, feat), lambda s, j, a, p=p: (head(p, s, j, a), 0, 0))
        )
        for n in range(SIDE):
            out_specs.append(
                pl.BlockSpec(
                    (1, srows, width),
                    lambda s, j, a, n=n: (
                        jnp.where(s < n, 0, jnp.where(s == n, j, SIDE - 1)),
                        0,
                        0,
                    ),
                )
            )
    states = pl.pallas_call(
        state_kernel,
        grid_spec=pltpu.PrefetchScalarGridSpec(
            num_scalar_prefetch=1,
            grid=(SIDE, SIDE),
            in_specs=in_specs,
            out_specs=out_specs,
        ),
        out_shape=[jax.ShapeDtypeStruct((SIDE, srows, width), BF16)] * (2 * SIDE),
        name="state",
    )(at, pk, pv, feat_k, pk, pv, feat_k)
    states = list(states)
    for p in range(2):
        for s in range(1, SIDE):
            i = SIDE * p + s
            states[i] = lax.ppermute(states[i], "dp", hop(s, 0) if p == 0 else hop(0, s))
    states = pl.pallas_call(
        add_kernel,
        in_specs=[pl.BlockSpec(memory_space=pltpu.SMEM)]
        + [pl.BlockSpec(memory_space=pltpu.VMEM)] * (2 * SIDE),
        out_shape=[jax.ShapeDtypeStruct((srows, width), BF16)] * (2 * SIDE),
        name="add",
    )(at, *states)
    states = list(states)
    for p in range(2):
        for s in range(1, SIDE):
            i = SIDE * p + s
            states[i] = lax.ppermute(states[i], "dp", hop(0, s) if p == 0 else hop(s, 0))

    inner = ()
    for p in range(2):
        specs = [pl.BlockSpec((length, width), lambda o, p=p: (0, 2 * o + p))] * 3
        specs += [pl.BlockSpec((1, width, feat), lambda o, p=p: (2 * o + p, 0, 0))] * 2
        inner = pl.pallas_call(
            intra_kernel,
            grid=(dp,),
            in_specs=specs + [pl.BlockSpec(memory_space=pl.ANY)] * p,
            out_specs=pl.BlockSpec((1, tall, width), lambda o, p=p: (o, 0, p)),
            out_shape=jax.ShapeDtypeStruct((dp, tall, two), BF16),
            input_output_aliases={5: 0} if p else {},
            name="intra",
        )(q, k, v, feat_q, feat_k, *inner)
        inner = (inner,)
    inner = lax.all_to_all(inner[0], "dp", 0, 0, tiled=True)

    total = dp * slots
    many = 4
    own_w = lax.dynamic_slice_in_dim(feat_q, 2 * me, 2, 0)
    row_spec = pl.BlockSpec((many, BLK, two), lambda i: (i, 0, 0))
    num, den = pl.pallas_call(
        prompt_kernel,
        grid=(total // many,),
        in_specs=[
            pl.BlockSpec(memory_space=pltpu.SMEM),
            pl.BlockSpec((dp, tall, two), lambda i: (0, 0, 0)),
            pl.BlockSpec((2, width, feat), lambda i: (0, 0, 0)),
        ]
        + [pl.BlockSpec((srows, width), lambda i: (0, 0))] * (2 * SIDE),
        out_specs=[row_spec, row_spec],
        out_shape=[jax.ShapeDtypeStruct((total, BLK, two), BF16)] * 2,
        scratch_shapes=[
            pltpu.VMEM((2, 2 * feat, width), BF16),
            pltpu.VMEM((2, width, 2 * feat), BF16),
        ],
        name="prompt",
    )(ids, q_all, own_w, *states)
    out = pl.pallas_call(
        combine_kernel,
        grid=(total // 8,),
        in_specs=[
            pl.BlockSpec(memory_space=pltpu.SMEM),
            pl.BlockSpec(memory_space=pltpu.SMEM),
            pl.BlockSpec((dp, tall, two), lambda i: (0, 0, 0)),
            pl.BlockSpec((8, BLK, two), lambda i: (i, 0, 0)),
            pl.BlockSpec((8, BLK, two), lambda i: (i, 0, 0)),
        ],
        out_specs=pl.BlockSpec((8 * BLK, two), lambda i: (i, 0)),
        out_shape=jax.ShapeDtypeStruct((total * BLK, two), BF16),
        name="combine",
    )(ids, lens, inner, num, den)
    out = lax.all_to_all(out.reshape(dp, slots * BLK, two), "dp", 0, 0, tiled=True)
    attn = pl.pallas_call(
        place_kernel,
        grid=(4,),
        in_specs=[pl.BlockSpec((dp // 4, slots * BLK, two), lambda i: (i, 0, 0))],
        out_specs=pl.BlockSpec((slots * BLK, heads * width // 4), lambda i: (0, i)),
        out_shape=jax.ShapeDtypeStruct((slots * BLK, heads * width), BF16),
        name="place",
    )(out)

    centred = reward_all - jnp.sum(reward_all) / dp
    spread = jnp.sum(centred * centred).reshape(1, 1)
    step = 1
    while step < groups:
        spread = spread + lax.ppermute(
            spread, "group", [(g, g ^ step) for g in range(groups)]
        )
        step *= 2
    advantage = centred / jnp.sqrt(spread[0, 0] / (groups * dp) + 1e-06)
    own = assign[0]
    picker = (own // pieces)[:, None] == jnp.arange(dp)[None, :]
    slot_adv = jnp.sum(jnp.where(picker, advantage[None, :], 0.0), axis=1)
    slot_len = jnp.sum(jnp.where(picker, lens[None, :], 0), axis=1)
    positions = (own % pieces)[:, None] * BLK + jnp.arange(BLK)[None, :]
    token_adv = jnp.where(positions < slot_len[:, None], slot_adv[:, None], F32(0.0))
    return (attn[None], token_adv.reshape(1, slots * BLK))


def solution(mesh):
    return jax.shard_map(
        body,
        mesh=mesh,
        in_specs=(
            P("group", "dp", None),
            P("group", "dp", None),
            P("group", "dp", None),
            P("group", "dp", None),
            P("group", "dp", None),
            P("group"),
            P("group", "dp"),
            P("group", "dp"),
            P("group", "dp"),
            P(),
            P(),
        ),
        out_specs=(P("group", "dp", None), P("group", "dp")),
        check_vma=False,
    )
```

```python
import jax
import jax.numpy as jnp
from jax import lax
from jax.experimental import pallas as pl
from jax.experimental.pallas import tpu as pltpu
from jax.sharding import PartitionSpec as P


BLK = 64
SIDE = 4
EXTRA = 8
F32 = jnp.float32
BF16 = jnp.bfloat16
NT = (((1,), (1,)), ((), ()))
TN = (((0,), (0,)), ((), ()))
NN = (((1,), (0,)), ((), ()))


def mm(a, b, dims=NN):
    return lax.dot_general(a, b, dims, preferred_element_type=F32)


def feats(xs, ws):
    us = [mm(w.T, x, NT) for x, w in zip(xs, ws)]
    top = [jnp.max(u, axis=0, keepdims=True) for u in us]
    low = [jnp.min(u, axis=0, keepdims=True) for u in us]
    ep = [jnp.exp(u - m) for u, m in zip(us, top)]
    en = [jnp.exp(m - u) for u, m in zip(us, low)]
    rp = [1.0 / jnp.sum(e, axis=0, keepdims=True) for e in ep]
    rn = [1.0 / jnp.sum(e, axis=0, keepdims=True) for e in en]
    return [
        jnp.concatenate([(a * b).astype(BF16), (c * d).astype(BF16)], axis=0)
        for a, b, c, d in zip(ep, rp, en, rn)
    ]


def spread_kernel(own_ref, len_ref, rew_ref, q_ref, o_ref):
    length, width = q_ref.shape[0], o_ref.shape[2]
    part = width // 8
    slots = own_ref.shape[1]
    col = lax.broadcasted_iota(jnp.int32, (EXTRA, width), 1)
    r = jnp.where(col < part, 0.0, rew_ref[0, 0])
    for i in range(slots):
        r = jnp.where(col == i, own_ref[0, i].astype(F32), r)
    r = jnp.where(col == slots, len_ref[0, 0].astype(F32), r)
    r1 = r.astype(BF16).astype(F32)
    r2 = (r - r1).astype(BF16).astype(F32)
    r3 = r - r1 - r2
    tabs = jnp.where(col < 2 * part, r1, jnp.where(col < 3 * part, r2, r3)).astype(BF16)
    for o in range(o_ref.shape[0]):
        o_ref[o, :length, :] = q_ref[:, o * width : (o + 1) * width]
        o_ref[o, length:, :] = tabs


def state_kernel(n_ref, k_ref, v_ref, w_ref, *outs):
    rows, width = k_ref.shape[0], w_ref.shape[1]
    half = w_ref.shape[2]
    me = lax.axis_index("dp")
    mx, my, j = me // SIDE, me % SIDE, pl.program_id(0)
    keep = lax.broadcasted_iota(jnp.int32, (1, rows), 1) + me * rows < n_ref[0]
    rid = lax.broadcasted_iota(jnp.int32, (EXTRA, rows), 0)
    heads = [2 * ((mx + s) % SIDE * SIDE + j) for s in range(SIDE)]
    heads += [2 * (j * SIDE + (my + s) % SIDE) + 1 for s in range(SIDE)]
    cols = [pl.ds(pl.multiple_of(h * width, width), width) for h in heads]
    phis = feats([k_ref[:, c] for c in cols], [w_ref[h] for h in heads])
    for phi, c, o_ref in zip(phis, cols, outs):
        phi = jnp.where(keep, phi, jnp.zeros((), BF16))
        o_ref[0, : 2 * half, :] = mm(phi, v_ref[:, c]).astype(BF16)
        tail = mm((rid == 0).astype(BF16), phi[:half], NT)
        tail = tail + mm((rid == 1).astype(BF16), phi[half:], NT)
        o_ref[0, 2 * half :, :] = tail.astype(BF16)


def add_kernel(*refs):
    ins, outs = refs[: 2 * SIDE], refs[2 * SIDE :]
    me = lax.axis_index("dp")
    for p in range(2):
        for s in range(SIDE):
            j = ((me // SIDE if p else me % SIDE) + s) % SIDE
            acc = ins[SIDE * p][j].astype(F32)
            for i in range(1, SIDE):
                acc = acc + ins[SIDE * p + i][j].astype(F32)
            outs[SIDE * p + s][...] = acc.astype(BF16)


def intra_kernel(q_ref, k_ref, v_ref, wq_ref, wk_ref, *rest):
    o_ref = rest[-1]
    length, width = q_ref.shape[0], wq_ref.shape[1]
    half = length // 2
    many = wq_ref.shape[0]
    cols = [slice(h * width, (h + 1) * width) for h in range(many)]
    phis = feats(
        [q_ref[:, c] for c in cols] + [k_ref[:, c] for c in cols],
        [wq_ref[h] for h in range(many)] + [wk_ref[h] for h in range(many)],
    )
    scores = [mm(phis[h].T, phis[many + h]) for h in range(many)]
    t = lax.broadcasted_iota(jnp.int32, (length, length), 0)
    s = lax.broadcasted_iota(jnp.int32, (length, length), 1)
    scores = [jnp.where(s <= t, x, 0.0) for x in scores]
    rid = lax.broadcasted_iota(jnp.int32, (EXTRA, half), 0)
    ones = jnp.ones((EXTRA, length), BF16)
    for h, score in enumerate(scores):
        to = slice(h % 2 * width, (h % 2 + 1) * width)
        num = mm(score.astype(BF16), v_ref[:, cols[h]])
        o_ref[h // 2, :length, to] = num.astype(BF16)
        fold = score[:, :half] + score[:, half:]
        hi = fold.astype(BF16)
        lo = (fold - hi.astype(F32)).astype(BF16)
        den = mm(ones, jnp.concatenate([hi, lo], axis=1), NT)
        den = jnp.where(rid < 2, den[:, :half], den[:, half:])
        dhi = den.astype(BF16).astype(F32)
        den = jnp.where(rid % 2 == 1, den - dhi, dhi)
        o_ref[h // 2, length:, to] = den.astype(BF16)


def prompt_kernel(ids_ref, q_ref, w_ref, *refs):
    parts = refs[: 2 * SIDE]
    num_ref, den_ref, s_ref, t_ref = refs[2 * SIDE :]
    i = pl.program_id(0)
    width = w_ref.shape[1]
    full = 2 * w_ref.shape[2]
    many = num_ref.shape[0]

    @pl.when(i == 0)
    def _():
        for h in range(2):
            acc = parts[SIDE * h][...].astype(F32)
            for d in range(1, SIDE):
                acc = acc + parts[SIDE * h + d][...].astype(F32)
            s_ref[h] = acc[:full].astype(BF16)
            row = jnp.concatenate([acc[full : full + 1], acc[full + 1 : full + 2]], axis=1)
            t_ref[h] = jnp.broadcast_to(row, t_ref.shape[1:]).astype(BF16)

    pieces = q_ref.shape[1] // BLK
    xs = []
    for g in range(0, many, 4):
        rows = []
        for j in range(g, g + 4):
            b = ids_ref[i * many + j]
            rows.append(q_ref[b // pieces, pl.ds(pl.multiple_of(b % pieces * BLK, BLK), BLK), :])
        xs.append(jnp.concatenate(rows, axis=0))
    cols = [slice(h * width, (h + 1) * width) for h in range(2)]
    units = [(g, h) for g in range(len(xs)) for h in range(2)]
    phis = feats([xs[g][:, cols[h]] for g, h in units], [w_ref[h] for g, h in units])
    phis = [phi.T for phi in phis]
    for phi, (g, h) in zip(phis, units):
        num = mm(phi, s_ref[h]).astype(BF16)
        den = mm(phi, t_ref[h], NT).astype(BF16)
        num_ref[4 * g : 4 * g + 4, :, cols[h]] = num.reshape(4, BLK, width)
        den_ref[4 * g : 4 * g + 4, :, cols[h]] = den.reshape(4, BLK, width)


def combine_kernel(ids_ref, len_ref, part_ref, num_ref, den_ref, o_ref):
    length = part_ref.shape[1] - EXTRA
    width = part_ref.shape[2] // 2
    pieces = length // BLK
    many = num_ref.shape[0]
    i = pl.program_id(0)
    rid = lax.broadcasted_iota(jnp.int32, (EXTRA, width), 0)
    row = lax.broadcasted_iota(jnp.int32, (BLK, 1), 0)
    for j in range(many):
        b = ids_ref[i * many + j]
        r, c = b // pieces, b % pieces
        pick = (rid // 2 == c // 2).astype(BF16)
        for h in range(2):
            cols = slice(h * width, (h + 1) * width)
            num = part_ref[r, pl.ds(pl.multiple_of(c * BLK, BLK), BLK), cols].astype(F32)
            den = mm(part_ref[r, length:, cols], pick, TN)
            den = jnp.where(c % 2 == 0, den[:BLK], den[BLK:])
            num = num_ref[j, :, cols].astype(F32) + num
            den = den_ref[j, :, cols].astype(F32) + den
            out = jnp.where(row < len_ref[r] - c * BLK, num / den, 0.0)
            o_ref[j * BLK : (j + 1) * BLK, cols] = out.astype(BF16)


def hop(dx, dy):
    return [
        (x * SIDE + y, (x + dx) % SIDE * SIDE + (y + dy) % SIDE)
        for x in range(SIDE)
        for y in range(SIDE)
    ]


def body(
    resp_q,
    resp_k,
    resp_v,
    prompt_k,
    prompt_v,
    prompt_len,
    resp_len,
    assign,
    rewards,
    feat_q,
    feat_k,
):
    dp = lax.axis_size("dp")
    groups = lax.axis_size("group")
    me = lax.axis_index("dp")
    heads, width, feat = feat_q.shape
    length = resp_q.shape[1]
    pieces = length // BLK
    slots = assign.shape[1]
    two = 2 * width
    tall = length + EXTRA
    q, k, v, pk, pv = resp_q[0], resp_k[0], resp_v[0], prompt_k[0], prompt_v[0]

    part = two // 8
    q_all = pl.pallas_call(
        spread_kernel,
        grid=(2,),
        in_specs=[pl.BlockSpec(memory_space=pltpu.SMEM)] * 3
        + [pl.BlockSpec((length, heads * width // 2), lambda o: (0, o))],
        out_specs=pl.BlockSpec((dp // 2, tall, two), lambda o: (o, 0, 0)),
        out_shape=jax.ShapeDtypeStruct((dp, tall, two), BF16),
        name="spread",
    )(assign, resp_len, rewards, q)
    q_all = lax.all_to_all(q_all, "dp", 0, 0, tiled=True)
    tabs = q_all[:, length, :].astype(F32)
    ids = tabs[:, :slots].astype(jnp.int32).reshape(-1)
    lens = tabs[:, slots].astype(jnp.int32)
    reward_all = tabs[:, part] + tabs[:, 2 * part] + tabs[:, 3 * part]

    srows = 2 * feat + EXTRA
    states = pl.pallas_call(
        state_kernel,
        grid=(SIDE,),
        in_specs=[
            pl.BlockSpec(memory_space=pltpu.SMEM),
            pl.BlockSpec(pk.shape, lambda j: (0, 0)),
            pl.BlockSpec(pv.shape, lambda j: (0, 0)),
            pl.BlockSpec(feat_k.shape, lambda j: (0, 0, 0)),
        ],
        out_specs=[pl.BlockSpec((1, srows, width), lambda j: (j, 0, 0))] * (2 * SIDE),
        out_shape=[jax.ShapeDtypeStruct((SIDE, srows, width), BF16)] * (2 * SIDE),
        name="state",
    )(prompt_len, pk, pv, feat_k)
    states = list(states)
    for p in range(2):
        for s in range(1, SIDE):
            i = SIDE * p + s
            states[i] = lax.ppermute(states[i], "dp", hop(s, 0) if p == 0 else hop(0, s))
    states = pl.pallas_call(
        add_kernel,
        in_specs=[pl.BlockSpec(memory_space=pltpu.VMEM)] * (2 * SIDE),
        out_shape=[jax.ShapeDtypeStruct((srows, width), BF16)] * (2 * SIDE),
        name="add",
    )(*states)
    states = list(states)
    for p in range(2):
        for s in range(1, SIDE):
            i = SIDE * p + s
            states[i] = lax.ppermute(states[i], "dp", hop(0, s) if p == 0 else hop(s, 0))

    inner = ()
    for p in range(2):
        at = p * (heads // 8)
        specs = [pl.BlockSpec((length, 4 * width), lambda o, at=at: (0, o + at))] * 3
        specs += [pl.BlockSpec((4, width, feat), lambda o, at=at: (o + at, 0, 0))] * 2
        inner = pl.pallas_call(
            intra_kernel,
            grid=(heads // 8,),
            in_specs=specs + [pl.BlockSpec(memory_space=pl.ANY)] * p,
            out_specs=pl.BlockSpec((2, tall, two), lambda o, at=at: (o + at, 0, 0)),
            out_shape=jax.ShapeDtypeStruct((dp, tall, two), BF16),
            input_output_aliases={5: 0} if p else {},
            name="intra",
        )(q, k, v, feat_q, feat_k, *inner)
        inner = (inner,)
    inner = lax.all_to_all(inner[0], "dp", 0, 0, tiled=True)

    total = dp * slots
    many = 8
    own_w = lax.dynamic_slice_in_dim(feat_q, 2 * me, 2, 0)
    row_spec = pl.BlockSpec((many, BLK, two), lambda i: (i, 0, 0))
    num, den = pl.pallas_call(
        prompt_kernel,
        grid=(total // many,),
        in_specs=[
            pl.BlockSpec(memory_space=pltpu.SMEM),
            pl.BlockSpec((dp, tall, two), lambda i: (0, 0, 0)),
            pl.BlockSpec((2, width, feat), lambda i: (0, 0, 0)),
        ]
        + [pl.BlockSpec((srows, width), lambda i: (0, 0))] * (2 * SIDE),
        out_specs=[row_spec, row_spec],
        out_shape=[jax.ShapeDtypeStruct((total, BLK, two), BF16)] * 2,
        scratch_shapes=[
            pltpu.VMEM((2, 2 * feat, width), BF16),
            pltpu.VMEM((2, width, 2 * feat), BF16),
        ],
        name="prompt",
    )(ids, q_all, own_w, *states)
    out = pl.pallas_call(
        combine_kernel,
        grid=(total // 8,),
        in_specs=[
            pl.BlockSpec(memory_space=pltpu.SMEM),
            pl.BlockSpec(memory_space=pltpu.SMEM),
            pl.BlockSpec((dp, tall, two), lambda i: (0, 0, 0)),
            pl.BlockSpec((8, BLK, two), lambda i: (i, 0, 0)),
            pl.BlockSpec((8, BLK, two), lambda i: (i, 0, 0)),
        ],
        out_specs=pl.BlockSpec((8 * BLK, two), lambda i: (i, 0)),
        out_shape=jax.ShapeDtypeStruct((total * BLK, two), BF16),
        name="combine",
    )(ids, lens, inner, num, den)
    out = lax.all_to_all(out.reshape(dp, slots * BLK, two), "dp", 0, 0, tiled=True)
    attn = jnp.swapaxes(out, 0, 1).reshape(1, slots * BLK, heads * width)

    centred = reward_all - jnp.sum(reward_all) / dp
    spread = jnp.sum(centred * centred).reshape(1, 1)
    step = 1
    while step < groups:
        total_sq = spread
        for i in range(1, 4):
            total_sq = total_sq + lax.ppermute(
                spread, "group", [(g, g ^ (step * i)) for g in range(groups)]
            )
        spread = total_sq
        step *= 4
    advantage = centred / jnp.sqrt(spread[0, 0] / (groups * dp) + 1e-06)
    own = assign[0]
    picker = (own // pieces)[:, None] == jnp.arange(dp)[None, :]
    slot_adv = jnp.sum(jnp.where(picker, advantage[None, :], 0.0), axis=1)
    slot_len = jnp.sum(jnp.where(picker, lens[None, :], 0), axis=1)
    positions = (own % pieces)[:, None] * BLK + jnp.arange(BLK)[None, :]
    token_adv = jnp.where(positions < slot_len[:, None], slot_adv[:, None], F32(0.0))
    return (attn, token_adv.reshape(1, slots * BLK))


def solution(mesh):
    return jax.shard_map(
        body,
        mesh=mesh,
        in_specs=(
            P("group", "dp", None),
            P("group", "dp", None),
            P("group", "dp", None),
            P("group", "dp", None),
            P("group", "dp", None),
            P("group"),
            P("group", "dp"),
            P("group", "dp"),
            P("group", "dp"),
            P(),
            P(),
        ),
        out_specs=(P("group", "dp", None), P("group", "dp")),
        check_vma=False,
    )
```

```python
import jax
import jax.numpy as jnp
from jax import lax
from jax.experimental import pallas as pl
from jax.experimental.pallas import tpu as pltpu
from jax.sharding import PartitionSpec as P


BLK = 64
SIDE = 4
EXTRA = 8
F32 = jnp.float32
BF16 = jnp.bfloat16
NT = (((1,), (1,)), ((), ()))
TN = (((0,), (0,)), ((), ()))
NN = (((1,), (0,)), ((), ()))


def mm(a, b, dims=NN):
    return lax.dot_general(a, b, dims, preferred_element_type=F32)


def feats(xs, ws):
    us = [mm(w.T, x, NT) for x, w in zip(xs, ws)]
    top = [jnp.max(u, axis=0, keepdims=True) for u in us]
    low = [jnp.min(u, axis=0, keepdims=True) for u in us]
    ep = [jnp.exp(u - m) for u, m in zip(us, top)]
    en = [jnp.exp(m - u) for u, m in zip(us, low)]
    rp = [1.0 / jnp.sum(e, axis=0, keepdims=True) for e in ep]
    rn = [1.0 / jnp.sum(e, axis=0, keepdims=True) for e in en]
    return [
        jnp.concatenate([(a * b).astype(BF16), (c * d).astype(BF16)], axis=0)
        for a, b, c, d in zip(ep, rp, en, rn)
    ]


def spread_kernel(own_ref, len_ref, rew_ref, q_ref, o_ref):
    length, width = q_ref.shape[0], o_ref.shape[2]
    part = width // 8
    slots = own_ref.shape[1]
    col = lax.broadcasted_iota(jnp.int32, (EXTRA, width), 1)
    r = jnp.where(col < part, 0.0, rew_ref[...])
    for i in range(slots):
        r = jnp.where(col == i, own_ref[:, i : i + 1].astype(F32), r)
    r = jnp.where(col == slots, len_ref[...].astype(F32), r)
    r1 = r.astype(BF16).astype(F32)
    r2 = (r - r1).astype(BF16).astype(F32)
    r3 = r - r1 - r2
    tabs = jnp.where(col < 2 * part, r1, jnp.where(col < 3 * part, r2, r3)).astype(BF16)
    for o in range(o_ref.shape[0]):
        o_ref[o, :length, :] = q_ref[:, o * width : (o + 1) * width]
        o_ref[o, length:, :] = tabs


def state_kernel(n_ref, k_ref, v_ref, w_ref, *outs):
    rows, width = k_ref.shape[0], w_ref.shape[1]
    half = w_ref.shape[2]
    me = lax.axis_index("dp")
    mx, my, j = me // SIDE, me % SIDE, pl.program_id(0)
    keep = lax.broadcasted_iota(jnp.int32, (1, rows), 1) + me * rows < n_ref[0]
    rid = lax.broadcasted_iota(jnp.int32, (EXTRA, rows), 0)
    heads = [2 * ((mx + s) % SIDE * SIDE + j) for s in range(SIDE)]
    heads += [2 * (j * SIDE + (my + s) % SIDE) + 1 for s in range(SIDE)]
    cols = [pl.ds(pl.multiple_of(h * width, width), width) for h in heads]
    phis = feats([k_ref[:, c] for c in cols], [w_ref[h] for h in heads])
    for phi, c, o_ref in zip(phis, cols, outs):
        phi = jnp.where(keep, phi, jnp.zeros((), BF16))
        o_ref[0, : 2 * half, :] = mm(phi, v_ref[:, c]).astype(BF16)
        tail = mm((rid == 0).astype(BF16), phi[:half], NT)
        tail = tail + mm((rid == 1).astype(BF16), phi[half:], NT)
        o_ref[0, 2 * half :, :] = tail.astype(BF16)


def add_kernel(*refs):
    ins, outs = refs[: 2 * SIDE], refs[2 * SIDE :]
    me = lax.axis_index("dp")
    for p in range(2):
        for s in range(SIDE):
            j = ((me // SIDE if p else me % SIDE) + s) % SIDE
            acc = ins[SIDE * p][j].astype(F32)
            for i in range(1, SIDE):
                acc = acc + ins[SIDE * p + i][j].astype(F32)
            outs[SIDE * p + s][...] = acc.astype(BF16)


def intra_kernel(q_ref, k_ref, v_ref, wq_ref, wk_ref, o_ref):
    length, width = q_ref.shape[0], wq_ref.shape[1]
    half = length // 2
    many = wq_ref.shape[0]
    cols = [slice(h * width, (h + 1) * width) for h in range(many)]
    phis = feats(
        [q_ref[:, c] for c in cols] + [k_ref[:, c] for c in cols],
        [wq_ref[h] for h in range(many)] + [wk_ref[h] for h in range(many)],
    )
    scores = [mm(phis[h].T, phis[many + h]) for h in range(many)]
    t = lax.broadcasted_iota(jnp.int32, (length, length), 0)
    s = lax.broadcasted_iota(jnp.int32, (length, length), 1)
    scores = [jnp.where(s <= t, x, 0.0) for x in scores]
    rid = lax.broadcasted_iota(jnp.int32, (EXTRA, half), 0)
    ones = jnp.ones((EXTRA, length), BF16)
    for h, score in enumerate(scores):
        to = slice(h % 2 * width, (h % 2 + 1) * width)
        num = mm(score.astype(BF16), v_ref[:, cols[h]])
        o_ref[h // 2, :length, to] = num.astype(BF16)
        fold = score[:, :half] + score[:, half:]
        hi = fold.astype(BF16)
        lo = (fold - hi.astype(F32)).astype(BF16)
        den = mm(ones, jnp.concatenate([hi, lo], axis=1), NT)
        den = jnp.where(rid < 2, den[:, :half], den[:, half:])
        dhi = den.astype(BF16).astype(F32)
        den = jnp.where(rid % 2 == 1, den - dhi, dhi)
        o_ref[h // 2, length:, to] = den.astype(BF16)


def prompt_kernel(ids_ref, q_ref, w_ref, *refs):
    parts = refs[: 2 * SIDE]
    num_ref, den_ref, s_ref, t_ref = refs[2 * SIDE :]
    i = pl.program_id(0)
    width = w_ref.shape[1]
    full = 2 * w_ref.shape[2]
    many = num_ref.shape[0]

    @pl.when(i == 0)
    def _():
        for h in range(2):
            acc = parts[SIDE * h][...].astype(F32)
            for d in range(1, SIDE):
                acc = acc + parts[SIDE * h + d][...].astype(F32)
            s_ref[h] = acc[:full].astype(BF16)
            row = jnp.concatenate([acc[full : full + 1], acc[full + 1 : full + 2]], axis=1)
            t_ref[h] = jnp.broadcast_to(row, t_ref.shape[1:]).astype(BF16)

    pieces = q_ref.shape[1] // BLK
    xs = []
    for g in range(0, many, 4):
        rows = []
        for j in range(g, g + 4):
            b = ids_ref[i * many + j]
            rows.append(q_ref[b // pieces, pl.ds(pl.multiple_of(b % pieces * BLK, BLK), BLK), :])
        xs.append(jnp.concatenate(rows, axis=0))
    cols = [slice(h * width, (h + 1) * width) for h in range(2)]
    units = [(g, h) for g in range(len(xs)) for h in range(2)]
    phis = feats([xs[g][:, cols[h]] for g, h in units], [w_ref[h] for g, h in units])
    phis = [phi.T for phi in phis]
    for phi, (g, h) in zip(phis, units):
        num = mm(phi, s_ref[h]).astype(BF16)
        den = mm(phi, t_ref[h], NT).astype(BF16)
        num_ref[4 * g : 4 * g + 4, :, cols[h]] = num.reshape(4, BLK, width)
        den_ref[4 * g : 4 * g + 4, :, cols[h]] = den.reshape(4, BLK, width)


def combine_kernel(ids_ref, len_ref, part_ref, num_ref, den_ref, o_ref):
    length = part_ref.shape[1] - EXTRA
    width = part_ref.shape[2] // 2
    pieces = length // BLK
    many = num_ref.shape[0]
    i = pl.program_id(0)
    rid = lax.broadcasted_iota(jnp.int32, (EXTRA, width), 0)
    row = lax.broadcasted_iota(jnp.int32, (BLK, 1), 0)
    for j in range(many):
        b = ids_ref[i * many + j]
        r, c = b // pieces, b % pieces
        pick = (rid // 2 == c // 2).astype(BF16)
        for h in range(2):
            cols = slice(h * width, (h + 1) * width)
            num = part_ref[r, pl.ds(pl.multiple_of(c * BLK, BLK), BLK), cols].astype(F32)
            den = mm(part_ref[r, length:, cols], pick, TN)
            den = jnp.where(c % 2 == 0, den[:BLK], den[BLK:])
            num = num_ref[j, :, cols].astype(F32) + num
            den = den_ref[j, :, cols].astype(F32) + den
            out = jnp.where(row < len_ref[r] - c * BLK, num / den, 0.0)
            o_ref[j * BLK : (j + 1) * BLK, cols] = out.astype(BF16)


def hop(dx, dy):
    return [
        (x * SIDE + y, (x + dx) % SIDE * SIDE + (y + dy) % SIDE)
        for x in range(SIDE)
        for y in range(SIDE)
    ]


def body(
    resp_q,
    resp_k,
    resp_v,
    prompt_k,
    prompt_v,
    prompt_len,
    resp_len,
    assign,
    rewards,
    feat_q,
    feat_k,
):
    dp = lax.axis_size("dp")
    groups = lax.axis_size("group")
    me = lax.axis_index("dp")
    heads, width, feat = feat_q.shape
    length = resp_q.shape[1]
    pieces = length // BLK
    slots = assign.shape[1]
    two = 2 * width
    tall = length + EXTRA
    q, k, v, pk, pv = resp_q[0], resp_k[0], resp_v[0], prompt_k[0], prompt_v[0]

    part = two // 8
    q_all = pl.pallas_call(
        spread_kernel,
        grid=(2,),
        in_specs=[
            pl.BlockSpec(assign.shape, lambda o: (0, 0)),
            pl.BlockSpec(resp_len.shape, lambda o: (0, 0)),
            pl.BlockSpec(rewards.shape, lambda o: (0, 0)),
            pl.BlockSpec((length, heads * width // 2), lambda o: (0, o)),
        ],
        out_specs=pl.BlockSpec((dp // 2, tall, two), lambda o: (o, 0, 0)),
        out_shape=jax.ShapeDtypeStruct((dp, tall, two), BF16),
        name="spread",
    )(assign, resp_len, rewards, q)
    q_all = lax.all_to_all(q_all, "dp", 0, 0, tiled=True)
    tabs = q_all[:, length, :].astype(F32)
    ids = tabs[:, :slots].astype(jnp.int32).reshape(-1)
    lens = tabs[:, slots].astype(jnp.int32)
    reward_all = tabs[:, part] + tabs[:, 2 * part] + tabs[:, 3 * part]

    srows = 2 * feat + EXTRA
    states = pl.pallas_call(
        state_kernel,
        grid=(SIDE,),
        in_specs=[
            pl.BlockSpec(memory_space=pltpu.SMEM),
            pl.BlockSpec(pk.shape, lambda j: (0, 0)),
            pl.BlockSpec(pv.shape, lambda j: (0, 0)),
            pl.BlockSpec(feat_k.shape, lambda j: (0, 0, 0)),
        ],
        out_specs=[pl.BlockSpec((1, srows, width), lambda j: (j, 0, 0))] * (2 * SIDE),
        out_shape=[jax.ShapeDtypeStruct((SIDE, srows, width), BF16)] * (2 * SIDE),
        name="state",
    )(prompt_len, pk, pv, feat_k)
    states = list(states)
    for p in range(2):
        for s in range(1, SIDE):
            i = SIDE * p + s
            states[i] = lax.ppermute(states[i], "dp", hop(s, 0) if p == 0 else hop(0, s))
    states = pl.pallas_call(
        add_kernel,
        in_specs=[pl.BlockSpec(memory_space=pltpu.VMEM)] * (2 * SIDE),
        out_shape=[jax.ShapeDtypeStruct((srows, width), BF16)] * (2 * SIDE),
        name="add",
    )(*states)
    states = list(states)
    for p in range(2):
        for s in range(1, SIDE):
            i = SIDE * p + s
            states[i] = lax.ppermute(states[i], "dp", hop(0, s) if p == 0 else hop(s, 0))

    inner = pl.pallas_call(
        intra_kernel,
        grid=(heads // 4,),
        in_specs=[pl.BlockSpec((length, 4 * width), lambda o: (0, o))] * 3
        + [pl.BlockSpec((4, width, feat), lambda o: (o, 0, 0))] * 2,
        out_specs=pl.BlockSpec((2, tall, two), lambda o: (o, 0, 0)),
        out_shape=jax.ShapeDtypeStruct((dp, tall, two), BF16),
        name="intra",
    )(q, k, v, feat_q, feat_k)
    inner = lax.all_to_all(inner, "dp", 0, 0, tiled=True)

    total = dp * slots
    many = 8
    own_w = lax.dynamic_slice_in_dim(feat_q, 2 * me, 2, 0)
    row_spec = pl.BlockSpec((many, BLK, two), lambda i: (i, 0, 0))
    num, den = pl.pallas_call(
        prompt_kernel,
        grid=(total // many,),
        in_specs=[
            pl.BlockSpec(memory_space=pltpu.SMEM),
            pl.BlockSpec((dp, tall, two), lambda i: (0, 0, 0)),
            pl.BlockSpec((2, width, feat), lambda i: (0, 0, 0)),
        ]
        + [pl.BlockSpec((srows, width), lambda i: (0, 0))] * (2 * SIDE),
        out_specs=[row_spec, row_spec],
        out_shape=[jax.ShapeDtypeStruct((total, BLK, two), BF16)] * 2,
        scratch_shapes=[
            pltpu.VMEM((2, 2 * feat, width), BF16),
            pltpu.VMEM((2, width, 2 * feat), BF16),
        ],
        name="prompt",
    )(ids, q_all, own_w, *states)
    out = pl.pallas_call(
        combine_kernel,
        grid=(total // 8,),
        in_specs=[
            pl.BlockSpec(memory_space=pltpu.SMEM),
            pl.BlockSpec(memory_space=pltpu.SMEM),
            pl.BlockSpec((dp, tall, two), lambda i: (0, 0, 0)),
            pl.BlockSpec((8, BLK, two), lambda i: (i, 0, 0)),
            pl.BlockSpec((8, BLK, two), lambda i: (i, 0, 0)),
        ],
        out_specs=pl.BlockSpec((8 * BLK, two), lambda i: (i, 0)),
        out_shape=jax.ShapeDtypeStruct((total * BLK, two), BF16),
        name="combine",
    )(ids, lens, inner, num, den)
    out = lax.all_to_all(out.reshape(dp, slots * BLK, two), "dp", 0, 0, tiled=True)
    attn = jnp.swapaxes(out, 0, 1).reshape(1, slots * BLK, heads * width)

    centred = reward_all - jnp.sum(reward_all) / dp
    spread = jnp.sum(centred * centred).reshape(1, 1)
    step = 1
    while step < groups:
        total_sq = spread
        for i in range(1, 4):
            total_sq = total_sq + lax.ppermute(
                spread, "group", [(g, g ^ (step * i)) for g in range(groups)]
            )
        spread = total_sq
        step *= 4
    advantage = centred / jnp.sqrt(spread[0, 0] / (groups * dp) + 1e-06)
    own = assign[0]
    picker = (own // pieces)[:, None] == jnp.arange(dp)[None, :]
    slot_adv = jnp.sum(jnp.where(picker, advantage[None, :], 0.0), axis=1)
    slot_len = jnp.sum(jnp.where(picker, lens[None, :], 0), axis=1)
    positions = (own % pieces)[:, None] * BLK + jnp.arange(BLK)[None, :]
    token_adv = jnp.where(positions < slot_len[:, None], slot_adv[:, None], F32(0.0))
    return (attn, token_adv.reshape(1, slots * BLK))


def solution(mesh):
    return jax.shard_map(
        body,
        mesh=mesh,
        in_specs=(
            P("group", "dp", None),
            P("group", "dp", None),
            P("group", "dp", None),
            P("group", "dp", None),
            P("group", "dp", None),
            P("group"),
            P("group", "dp"),
            P("group", "dp"),
            P("group", "dp"),
            P(),
            P(),
        ),
        out_specs=(P("group", "dp", None), P("group", "dp")),
        check_vma=False,
    )
```

```python
import jax
import jax.numpy as jnp
from jax import lax
from jax.experimental import pallas as pl
from jax.experimental.pallas import tpu as pltpu
from jax.sharding import PartitionSpec as P


BLK = 64
SIDE = 4
EXTRA = 8
F32 = jnp.float32
BF16 = jnp.bfloat16
NT = (((1,), (1,)), ((), ()))
TN = (((0,), (0,)), ((), ()))
NN = (((1,), (0,)), ((), ()))


def mm(a, b, dims=NN):
    return lax.dot_general(a, b, dims, preferred_element_type=F32)


def feats(xs, ws):
    us = [mm(w.T, x, NT) for x, w in zip(xs, ws)]
    top = [jnp.max(u, axis=0, keepdims=True) for u in us]
    low = [jnp.min(u, axis=0, keepdims=True) for u in us]
    ep = [jnp.exp(u - m) for u, m in zip(us, top)]
    en = [jnp.exp(m - u) for u, m in zip(us, low)]
    rp = [1.0 / jnp.sum(e, axis=0, keepdims=True) for e in ep]
    rn = [1.0 / jnp.sum(e, axis=0, keepdims=True) for e in en]
    return [
        jnp.concatenate([(a * b).astype(BF16), (c * d).astype(BF16)], axis=0)
        for a, b, c, d in zip(ep, rp, en, rn)
    ]


def spread_kernel(own_ref, len_ref, rew_ref, q_ref, o_ref):
    length, width = q_ref.shape[0], o_ref.shape[2]
    part = width // 8
    slots = own_ref.shape[1]
    col = lax.broadcasted_iota(jnp.int32, (EXTRA, width), 1)
    r = jnp.where(col < part, 0.0, rew_ref[...])
    for i in range(slots):
        r = jnp.where(col == i, own_ref[:, i : i + 1].astype(F32), r)
    r = jnp.where(col == slots, len_ref[...].astype(F32), r)
    r1 = r.astype(BF16).astype(F32)
    r2 = (r - r1).astype(BF16).astype(F32)
    r3 = r - r1 - r2
    tabs = jnp.where(col < 2 * part, r1, jnp.where(col < 3 * part, r2, r3)).astype(BF16)
    for o in range(o_ref.shape[0]):
        o_ref[o, :length, :] = q_ref[:, o * width : (o + 1) * width]
        o_ref[o, length:, :] = tabs


def state_kernel(n_ref, k_ref, v_ref, w_ref, *outs):
    rows, width = k_ref.shape[0], w_ref.shape[1]
    half = w_ref.shape[2]
    me = lax.axis_index("dp")
    mx, my, j = me // SIDE, me % SIDE, pl.program_id(0)
    keep = lax.broadcasted_iota(jnp.int32, (1, rows), 1) + me * rows < n_ref[0]
    rid = lax.broadcasted_iota(jnp.int32, (EXTRA, rows), 0)
    heads = [2 * ((mx + s) % SIDE * SIDE + j) for s in range(SIDE)]
    heads += [2 * (j * SIDE + (my + s) % SIDE) + 1 for s in range(SIDE)]
    cols = [pl.ds(pl.multiple_of(h * width, width), width) for h in heads]
    phis = feats([k_ref[:, c] for c in cols], [w_ref[h] for h in heads])
    for phi, c, o_ref in zip(phis, cols, outs):
        phi = jnp.where(keep, phi, jnp.zeros((), BF16))
        o_ref[0, : 2 * half, :] = mm(phi, v_ref[:, c]).astype(BF16)
        tail = mm((rid == 0).astype(BF16), phi[:half], NT)
        tail = tail + mm((rid == 1).astype(BF16), phi[half:], NT)
        o_ref[0, 2 * half :, :] = tail.astype(BF16)


def add_kernel(*refs):
    ins, outs = refs[: 2 * SIDE], refs[2 * SIDE :]
    me = lax.axis_index("dp")
    for p in range(2):
        for s in range(SIDE):
            j = ((me // SIDE if p else me % SIDE) + s) % SIDE
            acc = ins[SIDE * p][j].astype(F32)
            for i in range(1, SIDE):
                acc = acc + ins[SIDE * p + i][j].astype(F32)
            outs[SIDE * p + s][...] = acc.astype(BF16)


def intra_kernel(q_ref, k_ref, v_ref, wq_ref, wk_ref, o_ref):
    length, width = q_ref.shape[0], wq_ref.shape[1]
    half = length // 2
    many = wq_ref.shape[0]
    cols = [slice(h * width, (h + 1) * width) for h in range(many)]
    phis = feats(
        [q_ref[:, c] for c in cols] + [k_ref[:, c] for c in cols],
        [wq_ref[h] for h in range(many)] + [wk_ref[h] for h in range(many)],
    )
    scores = [mm(phis[h].T, phis[many + h]) for h in range(many)]
    t = lax.broadcasted_iota(jnp.int32, (length, length), 0)
    s = lax.broadcasted_iota(jnp.int32, (length, length), 1)
    scores = [jnp.where(s <= t, x, 0.0) for x in scores]
    rid = lax.broadcasted_iota(jnp.int32, (EXTRA, half), 0)
    ones = jnp.ones((EXTRA, length), BF16)
    for h, score in enumerate(scores):
        to = slice(h % 2 * width, (h % 2 + 1) * width)
        num = mm(score.astype(BF16), v_ref[:, cols[h]])
        o_ref[h // 2, :length, to] = num.astype(BF16)
        fold = score[:, :half] + score[:, half:]
        hi = fold.astype(BF16)
        lo = (fold - hi.astype(F32)).astype(BF16)
        den = mm(ones, jnp.concatenate([hi, lo], axis=1), NT)
        den = jnp.where(rid < 2, den[:, :half], den[:, half:])
        dhi = den.astype(BF16).astype(F32)
        den = jnp.where(rid % 2 == 1, den - dhi, dhi)
        o_ref[h // 2, length:, to] = den.astype(BF16)


def phi_kernel(ids_ref, q_ref, w_ref, o_ref):
    i = pl.program_id(0)
    me = lax.axis_index("dp")
    width = w_ref.shape[1]
    many = o_ref.shape[1] // BLK
    pieces = q_ref.shape[1] // BLK
    xs = []
    for g in range(0, many, 4):
        rows = []
        for j in range(g, g + 4):
            b = ids_ref[i * many + j]
            rows.append(q_ref[b // pieces, pl.ds(pl.multiple_of(b % pieces * BLK, BLK), BLK), :])
        xs.append(jnp.concatenate(rows, axis=0))
    units = [(g, h) for g in range(len(xs)) for h in range(2)]
    phis = feats(
        [xs[g][:, h * width : (h + 1) * width] for g, h in units],
        [w_ref[2 * me + h] for g, h in units],
    )
    for phi, (g, h) in zip(phis, units):
        o_ref[h, 4 * g * BLK : 4 * (g + 1) * BLK, :] = phi.T


def combine_kernel(ids_ref, len_ref, part_ref, phi_ref, *refs):
    parts = refs[: 2 * SIDE]
    o_ref, s_ref, t_ref = refs[2 * SIDE :]
    length = part_ref.shape[1] - EXTRA
    width = part_ref.shape[2] // 2
    full = phi_ref.shape[2]
    pieces = length // BLK
    many = phi_ref.shape[1] // BLK
    i = pl.program_id(0)

    @pl.when(i == 0)
    def _():
        for h in range(2):
            acc = parts[SIDE * h][...].astype(F32)
            for d in range(1, SIDE):
                acc = acc + parts[SIDE * h + d][...].astype(F32)
            s_ref[h] = acc[:full].astype(BF16)
            row = jnp.concatenate([acc[full : full + 1], acc[full + 1 : full + 2]], axis=1)
            t_ref[h] = jnp.broadcast_to(row, t_ref.shape[1:]).astype(BF16)

    nums = [mm(phi_ref[h], s_ref[h]).astype(BF16) for h in range(2)]
    dens = [mm(phi_ref[h], t_ref[h], NT).astype(BF16) for h in range(2)]
    rid = lax.broadcasted_iota(jnp.int32, (EXTRA, width), 0)
    row = lax.broadcasted_iota(jnp.int32, (BLK, 1), 0)
    for j in range(many):
        b = ids_ref[i * many + j]
        r, c = b // pieces, b % pieces
        pick = (rid // 2 == c // 2).astype(BF16)
        rows = slice(j * BLK, (j + 1) * BLK)
        for h in range(2):
            cols = slice(h * width, (h + 1) * width)
            num = part_ref[r, pl.ds(pl.multiple_of(c * BLK, BLK), BLK), cols].astype(F32)
            den = mm(part_ref[r, length:, cols], pick, TN)
            den = jnp.where(c % 2 == 0, den[:BLK], den[BLK:])
            num = nums[h][rows].astype(F32) + num
            den = dens[h][rows].astype(F32) + den
            out = jnp.where(row < len_ref[r] - c * BLK, num / den, 0.0)
            o_ref[rows, cols] = out.astype(BF16)


def hop(dx, dy):
    return [
        (x * SIDE + y, (x + dx) % SIDE * SIDE + (y + dy) % SIDE)
        for x in range(SIDE)
        for y in range(SIDE)
    ]


def body(
    resp_q,
    resp_k,
    resp_v,
    prompt_k,
    prompt_v,
    prompt_len,
    resp_len,
    assign,
    rewards,
    feat_q,
    feat_k,
):
    dp = lax.axis_size("dp")
    groups = lax.axis_size("group")
    heads, width, feat = feat_q.shape
    length = resp_q.shape[1]
    pieces = length // BLK
    slots = assign.shape[1]
    two = 2 * width
    tall = length + EXTRA
    q, k, v, pk, pv = resp_q[0], resp_k[0], resp_v[0], prompt_k[0], prompt_v[0]

    part = two // 8
    q_all = pl.pallas_call(
        spread_kernel,
        grid=(2,),
        in_specs=[
            pl.BlockSpec(assign.shape, lambda o: (0, 0)),
            pl.BlockSpec(resp_len.shape, lambda o: (0, 0)),
            pl.BlockSpec(rewards.shape, lambda o: (0, 0)),
            pl.BlockSpec((length, heads * width // 2), lambda o: (0, o)),
        ],
        out_specs=pl.BlockSpec((dp // 2, tall, two), lambda o: (o, 0, 0)),
        out_shape=jax.ShapeDtypeStruct((dp, tall, two), BF16),
        name="spread",
    )(assign, resp_len, rewards, q)
    q_all = lax.all_to_all(q_all, "dp", 0, 0, tiled=True)
    tabs = q_all[:, length, :].astype(F32)
    ids = tabs[:, :slots].astype(jnp.int32).reshape(-1)
    lens = tabs[:, slots].astype(jnp.int32)
    reward_all = tabs[:, part] + tabs[:, 2 * part] + tabs[:, 3 * part]

    srows = 2 * feat + EXTRA
    states = pl.pallas_call(
        state_kernel,
        grid=(SIDE,),
        in_specs=[
            pl.BlockSpec(memory_space=pltpu.SMEM),
            pl.BlockSpec(pk.shape, lambda j: (0, 0)),
            pl.BlockSpec(pv.shape, lambda j: (0, 0)),
            pl.BlockSpec(feat_k.shape, lambda j: (0, 0, 0)),
        ],
        out_specs=[pl.BlockSpec((1, srows, width), lambda j: (j, 0, 0))] * (2 * SIDE),
        out_shape=[jax.ShapeDtypeStruct((SIDE, srows, width), BF16)] * (2 * SIDE),
        name="state",
    )(prompt_len, pk, pv, feat_k)
    states = list(states)
    for p in range(2):
        for s in range(1, SIDE):
            i = SIDE * p + s
            states[i] = lax.ppermute(states[i], "dp", hop(s, 0) if p == 0 else hop(0, s))
    states = pl.pallas_call(
        add_kernel,
        in_specs=[pl.BlockSpec(memory_space=pltpu.VMEM)] * (2 * SIDE),
        out_shape=[jax.ShapeDtypeStruct((srows, width), BF16)] * (2 * SIDE),
        name="add",
    )(*states)
    states = list(states)
    for p in range(2):
        for s in range(1, SIDE):
            i = SIDE * p + s
            states[i] = lax.ppermute(states[i], "dp", hop(0, s) if p == 0 else hop(s, 0))

    inner = pl.pallas_call(
        intra_kernel,
        grid=(heads // 4,),
        in_specs=[pl.BlockSpec((length, 4 * width), lambda o: (0, o))] * 3
        + [pl.BlockSpec((4, width, feat), lambda o: (o, 0, 0))] * 2,
        out_specs=pl.BlockSpec((2, tall, two), lambda o: (o, 0, 0)),
        out_shape=jax.ShapeDtypeStruct((dp, tall, two), BF16),
        name="intra",
    )(q, k, v, feat_q, feat_k)
    inner = lax.all_to_all(inner, "dp", 0, 0, tiled=True)

    total = dp * slots
    many = 8
    phi = pl.pallas_call(
        phi_kernel,
        grid=(total // many,),
        in_specs=[
            pl.BlockSpec(memory_space=pltpu.SMEM),
            pl.BlockSpec((dp, tall, two), lambda i: (0, 0, 0)),
            pl.BlockSpec(feat_q.shape, lambda i: (0, 0, 0)),
        ],
        out_specs=pl.BlockSpec((2, many * BLK, 2 * feat), lambda i: (0, i, 0)),
        out_shape=jax.ShapeDtypeStruct((2, total * BLK, 2 * feat), BF16),
        name="phi",
    )(ids, q_all, feat_q)
    out = pl.pallas_call(
        combine_kernel,
        grid=(total // many,),
        in_specs=[
            pl.BlockSpec(memory_space=pltpu.SMEM),
            pl.BlockSpec(memory_space=pltpu.SMEM),
            pl.BlockSpec((dp, tall, two), lambda i: (0, 0, 0)),
            pl.BlockSpec((2, many * BLK, 2 * feat), lambda i: (0, i, 0)),
        ]
        + [pl.BlockSpec((srows, width), lambda i: (0, 0))] * (2 * SIDE),
        out_specs=pl.BlockSpec((many * BLK, two), lambda i: (i, 0)),
        out_shape=jax.ShapeDtypeStruct((total * BLK, two), BF16),
        scratch_shapes=[
            pltpu.VMEM((2, 2 * feat, width), BF16),
            pltpu.VMEM((2, width, 2 * feat), BF16),
        ],
        name="combine",
    )(ids, lens, inner, phi, *states)
    out = lax.all_to_all(out.reshape(dp, slots * BLK, two), "dp", 0, 0, tiled=True)
    attn = jnp.swapaxes(out, 0, 1).reshape(1, slots * BLK, heads * width)

    centred = reward_all - jnp.sum(reward_all) / dp
    spread = jnp.sum(centred * centred).reshape(1, 1)
    step = 1
    while step < groups:
        total_sq = spread
        for i in range(1, 4):
            total_sq = total_sq + lax.ppermute(
                spread, "group", [(g, g ^ (step * i)) for g in range(groups)]
            )
        spread = total_sq
        step *= 4
    advantage = centred / jnp.sqrt(spread[0, 0] / (groups * dp) + 1e-06)
    own = assign[0]
    picker = (own // pieces)[:, None] == jnp.arange(dp)[None, :]
    slot_adv = jnp.sum(jnp.where(picker, advantage[None, :], 0.0), axis=1)
    slot_len = jnp.sum(jnp.where(picker, lens[None, :], 0), axis=1)
    positions = (own % pieces)[:, None] * BLK + jnp.arange(BLK)[None, :]
    token_adv = jnp.where(positions < slot_len[:, None], slot_adv[:, None], F32(0.0))
    return (attn, token_adv.reshape(1, slots * BLK))


def solution(mesh):
    return jax.shard_map(
        body,
        mesh=mesh,
        in_specs=(
            P("group", "dp", None),
            P("group", "dp", None),
            P("group", "dp", None),
            P("group", "dp", None),
            P("group", "dp", None),
            P("group"),
            P("group", "dp"),
            P("group", "dp"),
            P("group", "dp"),
            P(),
            P(),
        ),
        out_specs=(P("group", "dp", None), P("group", "dp")),
        check_vma=False,
    )
```

```python
import jax
import jax.numpy as jnp
from jax import lax
from jax.experimental import pallas as pl
from jax.experimental.pallas import tpu as pltpu
from jax.sharding import PartitionSpec as P


BLK = 64
SIDE = 4
EXTRA = 8
F32 = jnp.float32
BF16 = jnp.bfloat16
NT = (((1,), (1,)), ((), ()))
TN = (((0,), (0,)), ((), ()))
NN = (((1,), (0,)), ((), ()))


def mm(a, b, dims=NN):
    return lax.dot_general(a, b, dims, preferred_element_type=F32)


def feats(xs, ws):
    us = [mm(w.T, x, NT) for x, w in zip(xs, ws)]
    top = [jnp.max(u, axis=0, keepdims=True) for u in us]
    low = [jnp.min(u, axis=0, keepdims=True) for u in us]
    ep = [jnp.exp(u - m) for u, m in zip(us, top)]
    en = [jnp.exp(m - u) for u, m in zip(us, low)]
    rp = [1.0 / jnp.sum(e, axis=0, keepdims=True) for e in ep]
    rn = [1.0 / jnp.sum(e, axis=0, keepdims=True) for e in en]
    return [
        jnp.concatenate([(a * b).astype(BF16), (c * d).astype(BF16)], axis=0)
        for a, b, c, d in zip(ep, rp, en, rn)
    ]


def spread_kernel(own_ref, len_ref, rew_ref, q_ref, o_ref):
    length, width = q_ref.shape[0], o_ref.shape[2]
    part = width // 8
    slots = own_ref.shape[1]
    col = lax.broadcasted_iota(jnp.int32, (EXTRA, width), 1)
    r = jnp.where(col < part, 0.0, rew_ref[...])
    for i in range(slots):
        r = jnp.where(col == i, own_ref[:, i : i + 1].astype(F32), r)
    r = jnp.where(col == slots, len_ref[...].astype(F32), r)
    r1 = r.astype(BF16).astype(F32)
    r2 = (r - r1).astype(BF16).astype(F32)
    r3 = r - r1 - r2
    tabs = jnp.where(col < 2 * part, r1, jnp.where(col < 3 * part, r2, r3)).astype(BF16)
    for o in range(o_ref.shape[0]):
        o_ref[o, :length, :] = q_ref[:, o * width : (o + 1) * width]
        o_ref[o, length:, :] = tabs


def state_kernel(n_ref, k_ref, v_ref, w_ref, *outs):
    rows, width = k_ref.shape[0], w_ref.shape[1]
    half = w_ref.shape[2]
    me = lax.axis_index("dp")
    mx, my, j = me // SIDE, me % SIDE, pl.program_id(0)
    keep = lax.broadcasted_iota(jnp.int32, (1, rows), 1) + me * rows < n_ref[0]
    rid = lax.broadcasted_iota(jnp.int32, (EXTRA, rows), 0)
    heads = [2 * ((mx + s) % SIDE * SIDE + j) for s in range(SIDE)]
    heads += [2 * (j * SIDE + (my + s) % SIDE) + 1 for s in range(SIDE)]
    cols = [pl.ds(pl.multiple_of(h * width, width), width) for h in heads]
    phis = feats([k_ref[:, c] for c in cols], [w_ref[h] for h in heads])
    for phi, c, o_ref in zip(phis, cols, outs):
        phi = jnp.where(keep, phi, jnp.zeros((), BF16))
        o_ref[0, : 2 * half, :] = mm(phi, v_ref[:, c]).astype(BF16)
        tail = mm((rid == 0).astype(BF16), phi[:half], NT)
        tail = tail + mm((rid == 1).astype(BF16), phi[half:], NT)
        o_ref[0, 2 * half :, :] = tail.astype(BF16)


def add_kernel(*refs):
    ins, outs = refs[: 2 * SIDE], refs[2 * SIDE :]
    me = lax.axis_index("dp")
    for p in range(2):
        for s in range(SIDE):
            j = ((me // SIDE if p else me % SIDE) + s) % SIDE
            acc = ins[SIDE * p][j].astype(F32)
            for i in range(1, SIDE):
                acc = acc + ins[SIDE * p + i][j].astype(F32)
            outs[SIDE * p + s][...] = acc.astype(BF16)


def intra_kernel(q_ref, k_ref, v_ref, wq_ref, wk_ref, o_ref):
    length, width = q_ref.shape[0], wq_ref.shape[1]
    half = length // 2
    many = wq_ref.shape[0]
    cols = [slice(h * width, (h + 1) * width) for h in range(many)]
    phis = feats(
        [q_ref[:, c] for c in cols] + [k_ref[:, c] for c in cols],
        [wq_ref[h] for h in range(many)] + [wk_ref[h] for h in range(many)],
    )
    scores = [mm(phis[h].T, phis[many + h]) for h in range(many)]
    t = lax.broadcasted_iota(jnp.int32, (length, length), 0)
    s = lax.broadcasted_iota(jnp.int32, (length, length), 1)
    scores = [jnp.where(s <= t, x, 0.0) for x in scores]
    rid = lax.broadcasted_iota(jnp.int32, (EXTRA, half), 0)
    ones = jnp.ones((EXTRA, length), BF16)
    for h, score in enumerate(scores):
        to = slice(h % 2 * width, (h % 2 + 1) * width)
        num = mm(score.astype(BF16), v_ref[:, cols[h]])
        o_ref[h // 2, :length, to] = num.astype(BF16)
        fold = score[:, :half] + score[:, half:]
        hi = fold.astype(BF16)
        lo = (fold - hi.astype(F32)).astype(BF16)
        den = mm(ones, jnp.concatenate([hi, lo], axis=1), NT)
        den = jnp.where(rid < 2, den[:, :half], den[:, half:])
        dhi = den.astype(BF16).astype(F32)
        den = jnp.where(rid % 2 == 1, den - dhi, dhi)
        o_ref[h // 2, length:, to] = den.astype(BF16)


def phi_kernel(ids_ref, q_ref, w_ref, o_ref):
    i = pl.program_id(0)
    me = lax.axis_index("dp")
    width = w_ref.shape[1]
    many = o_ref.shape[1] // BLK
    pieces = q_ref.shape[1] // BLK
    xs = []
    for g in range(0, many, 4):
        rows = []
        for j in range(g, g + 4):
            b = ids_ref[i * many + j]
            rows.append(q_ref[b // pieces, pl.ds(pl.multiple_of(b % pieces * BLK, BLK), BLK), :])
        xs.append(jnp.concatenate(rows, axis=0))
    units = [(g, h) for g in range(len(xs)) for h in range(2)]
    phis = feats(
        [xs[g][:, h * width : (h + 1) * width] for g, h in units],
        [w_ref[2 * me + h] for g, h in units],
    )
    for phi, (g, h) in zip(phis, units):
        o_ref[h, 4 * g * BLK : 4 * (g + 1) * BLK, :] = phi.T


def combine_kernel(ids_ref, len_ref, sq_ref, part_ref, phi_ref, *refs):
    parts = refs[: 2 * SIDE]
    o_ref, s_ref, t_ref = refs[2 * SIDE :]
    length = part_ref.shape[1] - EXTRA
    width = part_ref.shape[2] // 2
    full = phi_ref.shape[2]
    pieces = length // BLK
    many = phi_ref.shape[1] // BLK
    i = pl.program_id(0)

    @pl.when(i == 0)
    def _():
        for h in range(2):
            acc = parts[SIDE * h][...].astype(F32)
            for d in range(1, SIDE):
                acc = acc + parts[SIDE * h + d][...].astype(F32)
            s_ref[h] = acc[:full].astype(BF16)
            row = jnp.concatenate([acc[full : full + 1], acc[full + 1 : full + 2]], axis=1)
            t_ref[h] = jnp.broadcast_to(row, t_ref.shape[1:]).astype(BF16)

    per = (o_ref.shape[1] - EXTRA) // BLK
    cut = 2 * width // 8
    col = lax.broadcasted_iota(jnp.int32, (EXTRA, 2 * width), 1)
    r = jnp.broadcast_to(sq_ref[...], col.shape)
    r1 = r.astype(BF16).astype(F32)
    r2 = (r - r1).astype(BF16).astype(F32)
    r3 = r - r1 - r2
    low = jnp.where(col < cut, r1, jnp.where(col < 2 * cut, r2, r3)).astype(BF16)
    for d in range(o_ref.shape[0]):
        o_ref[d, per * BLK :, :] = low
    nums = [mm(phi_ref[h], s_ref[h]).astype(BF16) for h in range(2)]
    dens = [mm(phi_ref[h], t_ref[h], NT).astype(BF16) for h in range(2)]
    rid = lax.broadcasted_iota(jnp.int32, (EXTRA, width), 0)
    row = lax.broadcasted_iota(jnp.int32, (BLK, 1), 0)
    for j in range(many):
        b = ids_ref[i * many + j]
        r, c = b // pieces, b % pieces
        pick = (rid // 2 == c // 2).astype(BF16)
        rows = slice(j * BLK, (j + 1) * BLK)
        for h in range(2):
            cols = slice(h * width, (h + 1) * width)
            num = part_ref[r, pl.ds(pl.multiple_of(c * BLK, BLK), BLK), cols].astype(F32)
            den = mm(part_ref[r, length:, cols], pick, TN)
            den = jnp.where(c % 2 == 0, den[:BLK], den[BLK:])
            num = nums[h][rows].astype(F32) + num
            den = dens[h][rows].astype(F32) + den
            out = jnp.where(row < len_ref[r] - c * BLK, num / den, 0.0)
            o_ref[j // per, j % per * BLK : (j % per + 1) * BLK, cols] = out.astype(BF16)


def hop(dx, dy):
    return [
        (x * SIDE + y, (x + dx) % SIDE * SIDE + (y + dy) % SIDE)
        for x in range(SIDE)
        for y in range(SIDE)
    ]


def body(
    resp_q,
    resp_k,
    resp_v,
    prompt_k,
    prompt_v,
    prompt_len,
    resp_len,
    assign,
    rewards,
    feat_q,
    feat_k,
):
    dp = lax.axis_size("dp")
    groups = lax.axis_size("group")
    heads, width, feat = feat_q.shape
    length = resp_q.shape[1]
    pieces = length // BLK
    slots = assign.shape[1]
    two = 2 * width
    tall = length + EXTRA
    q, k, v, pk, pv = resp_q[0], resp_k[0], resp_v[0], prompt_k[0], prompt_v[0]

    part = two // 8
    q_all = pl.pallas_call(
        spread_kernel,
        grid=(2,),
        in_specs=[
            pl.BlockSpec(assign.shape, lambda o: (0, 0)),
            pl.BlockSpec(resp_len.shape, lambda o: (0, 0)),
            pl.BlockSpec(rewards.shape, lambda o: (0, 0)),
            pl.BlockSpec((length, heads * width // 2), lambda o: (0, o)),
        ],
        out_specs=pl.BlockSpec((dp // 2, tall, two), lambda o: (o, 0, 0)),
        out_shape=jax.ShapeDtypeStruct((dp, tall, two), BF16),
        name="spread",
    )(assign, resp_len, rewards, q)
    q_all = lax.all_to_all(q_all, "dp", 0, 0, tiled=True)
    tabs = q_all[:, length, :].astype(F32)
    ids = tabs[:, :slots].astype(jnp.int32).reshape(-1)
    lens = tabs[:, slots].astype(jnp.int32)
    reward_all = tabs[:, part] + tabs[:, 2 * part] + tabs[:, 3 * part]

    srows = 2 * feat + EXTRA
    states = pl.pallas_call(
        state_kernel,
        grid=(SIDE,),
        in_specs=[
            pl.BlockSpec(memory_space=pltpu.SMEM),
            pl.BlockSpec(pk.shape, lambda j: (0, 0)),
            pl.BlockSpec(pv.shape, lambda j: (0, 0)),
            pl.BlockSpec(feat_k.shape, lambda j: (0, 0, 0)),
        ],
        out_specs=[pl.BlockSpec((1, srows, width), lambda j: (j, 0, 0))] * (2 * SIDE),
        out_shape=[jax.ShapeDtypeStruct((SIDE, srows, width), BF16)] * (2 * SIDE),
        name="state",
    )(prompt_len, pk, pv, feat_k)
    states = list(states)
    for p in range(2):
        for s in range(1, SIDE):
            i = SIDE * p + s
            states[i] = lax.ppermute(states[i], "dp", hop(s, 0) if p == 0 else hop(0, s))
    states = pl.pallas_call(
        add_kernel,
        in_specs=[pl.BlockSpec(memory_space=pltpu.VMEM)] * (2 * SIDE),
        out_shape=[jax.ShapeDtypeStruct((srows, width), BF16)] * (2 * SIDE),
        name="add",
    )(*states)
    states = list(states)
    for p in range(2):
        for s in range(1, SIDE):
            i = SIDE * p + s
            states[i] = lax.ppermute(states[i], "dp", hop(0, s) if p == 0 else hop(s, 0))

    inner = pl.pallas_call(
        intra_kernel,
        grid=(heads // 4,),
        in_specs=[pl.BlockSpec((length, 4 * width), lambda o: (0, o))] * 3
        + [pl.BlockSpec((4, width, feat), lambda o: (o, 0, 0))] * 2,
        out_specs=pl.BlockSpec((2, tall, two), lambda o: (o, 0, 0)),
        out_shape=jax.ShapeDtypeStruct((dp, tall, two), BF16),
        name="intra",
    )(q, k, v, feat_q, feat_k)
    inner = lax.all_to_all(inner, "dp", 0, 0, tiled=True)

    centred = reward_all - jnp.sum(reward_all) / dp
    squares = lax.ppermute(
        jnp.sum(centred * centred).reshape(1, 1),
        ("group", "dp"),
        [(g * dp + d, (g + d) % groups * dp + d) for g in range(groups) for d in range(dp)],
    )

    short = slots * BLK + EXTRA
    total = dp * slots
    many = 8
    phi = pl.pallas_call(
        phi_kernel,
        grid=(total // many,),
        in_specs=[
            pl.BlockSpec(memory_space=pltpu.SMEM),
            pl.BlockSpec((dp, tall, two), lambda i: (0, 0, 0)),
            pl.BlockSpec(feat_q.shape, lambda i: (0, 0, 0)),
        ],
        out_specs=pl.BlockSpec((2, many * BLK, 2 * feat), lambda i: (0, i, 0)),
        out_shape=jax.ShapeDtypeStruct((2, total * BLK, 2 * feat), BF16),
        name="phi",
    )(ids, q_all, feat_q)
    out = pl.pallas_call(
        combine_kernel,
        grid=(total // many,),
        in_specs=[
            pl.BlockSpec(memory_space=pltpu.SMEM),
            pl.BlockSpec(memory_space=pltpu.SMEM),
            pl.BlockSpec((1, 1), lambda i: (0, 0)),
            pl.BlockSpec((dp, tall, two), lambda i: (0, 0, 0)),
            pl.BlockSpec((2, many * BLK, 2 * feat), lambda i: (0, i, 0)),
        ]
        + [pl.BlockSpec((srows, width), lambda i: (0, 0))] * (2 * SIDE),
        out_specs=pl.BlockSpec((many // slots, short, two), lambda i: (i, 0, 0)),
        out_shape=jax.ShapeDtypeStruct((dp, short, two), BF16),
        scratch_shapes=[
            pltpu.VMEM((2, 2 * feat, width), BF16),
            pltpu.VMEM((2, width, 2 * feat), BF16),
        ],
        name="combine",
    )(ids, lens, squares, inner, phi, *states)
    out = lax.all_to_all(out, "dp", 0, 0, tiled=True)
    attn = jnp.swapaxes(out[:, : slots * BLK], 0, 1).reshape(1, slots * BLK, heads * width)

    squares = out[:, slots * BLK, :].astype(F32)
    spread = jnp.sum(squares[:, 0] + squares[:, part] + squares[:, 2 * part])
    advantage = centred / jnp.sqrt(spread / (groups * dp) + 1e-06)
    own = assign[0]
    picker = (own // pieces)[:, None] == jnp.arange(dp)[None, :]
    slot_adv = jnp.sum(jnp.where(picker, advantage[None, :], 0.0), axis=1)
    slot_len = jnp.sum(jnp.where(picker, lens[None, :], 0), axis=1)
    positions = (own % pieces)[:, None] * BLK + jnp.arange(BLK)[None, :]
    token_adv = jnp.where(positions < slot_len[:, None], slot_adv[:, None], F32(0.0))
    return (attn, token_adv.reshape(1, slots * BLK))


def solution(mesh):
    return jax.shard_map(
        body,
        mesh=mesh,
        in_specs=(
            P("group", "dp", None),
            P("group", "dp", None),
            P("group", "dp", None),
            P("group", "dp", None),
            P("group", "dp", None),
            P("group"),
            P("group", "dp"),
            P("group", "dp"),
            P("group", "dp"),
            P(),
            P(),
        ),
        out_specs=(P("group", "dp", None), P("group", "dp")),
        check_vma=False,
    )
```

```python
import jax
import jax.numpy as jnp
from jax import lax
from jax.experimental import pallas as pl
from jax.experimental.pallas import tpu as pltpu
from jax.sharding import PartitionSpec as P


BLK = 64
SIDE = 4
EXTRA = 8
F32 = jnp.float32
BF16 = jnp.bfloat16
NT = (((1,), (1,)), ((), ()))
TN = (((0,), (0,)), ((), ()))
NN = (((1,), (0,)), ((), ()))


def mm(a, b, dims=NN):
    return lax.dot_general(a, b, dims, preferred_element_type=F32)


def feats(xs, ws):
    us = [mm(w.T, x, NT) for x, w in zip(xs, ws)]
    top = [jnp.max(u, axis=0, keepdims=True) for u in us]
    low = [jnp.min(u, axis=0, keepdims=True) for u in us]
    ep = [jnp.exp(u - m) for u, m in zip(us, top)]
    en = [jnp.exp(m - u) for u, m in zip(us, low)]
    rp = [1.0 / jnp.sum(e, axis=0, keepdims=True) for e in ep]
    rn = [1.0 / jnp.sum(e, axis=0, keepdims=True) for e in en]
    return [
        jnp.concatenate([(a * b).astype(BF16), (c * d).astype(BF16)], axis=0)
        for a, b, c, d in zip(ep, rp, en, rn)
    ]


def spread_kernel(own_ref, len_ref, rew_ref, q_ref, o_ref):
    length, width = q_ref.shape[0], o_ref.shape[2]
    part = width // 8
    slots = own_ref.shape[1]
    col = lax.broadcasted_iota(jnp.int32, (EXTRA, width), 1)
    r = jnp.where(col < part, 0.0, rew_ref[...])
    for i in range(slots):
        r = jnp.where(col == i, own_ref[:, i : i + 1].astype(F32), r)
    r = jnp.where(col == slots, len_ref[...].astype(F32), r)
    r1 = r.astype(BF16).astype(F32)
    r2 = (r - r1).astype(BF16).astype(F32)
    r3 = r - r1 - r2
    tabs = jnp.where(col < 2 * part, r1, jnp.where(col < 3 * part, r2, r3)).astype(BF16)
    for o in range(o_ref.shape[0]):
        o_ref[o, :length, :] = q_ref[:, o * width : (o + 1) * width]
        o_ref[o, length:, :] = tabs


def state_kernel(n_ref, k_ref, v_ref, w_ref, *outs):
    rows, width = k_ref.shape[0], w_ref.shape[1]
    half = w_ref.shape[2]
    me = lax.axis_index("dp")
    mx, my, j = me // SIDE, me % SIDE, pl.program_id(0)
    keep = lax.broadcasted_iota(jnp.int32, (1, rows), 1) + me * rows < n_ref[0]
    rid = lax.broadcasted_iota(jnp.int32, (EXTRA, rows), 0)
    heads = [2 * ((mx + s) % SIDE * SIDE + j) for s in range(SIDE)]
    heads += [2 * (j * SIDE + (my + s) % SIDE) + 1 for s in range(SIDE)]
    cols = [pl.ds(pl.multiple_of(h * width, width), width) for h in heads]
    phis = feats([k_ref[:, c] for c in cols], [w_ref[h] for h in heads])
    for phi, c, o_ref in zip(phis, cols, outs):
        phi = jnp.where(keep, phi, jnp.zeros((), BF16))
        o_ref[0, : 2 * half, :] = mm(phi, v_ref[:, c]).astype(BF16)
        tail = mm((rid == 0).astype(BF16), phi[:half], NT)
        tail = tail + mm((rid == 1).astype(BF16), phi[half:], NT)
        o_ref[0, 2 * half :, :] = tail.astype(BF16)


def add_kernel(*refs):
    ins, outs = refs[: 2 * SIDE], refs[2 * SIDE :]
    me = lax.axis_index("dp")
    for p in range(2):
        for s in range(SIDE):
            j = ((me // SIDE if p else me % SIDE) + s) % SIDE
            acc = ins[SIDE * p][j].astype(F32)
            for i in range(1, SIDE):
                acc = acc + ins[SIDE * p + i][j].astype(F32)
            outs[SIDE * p + s][...] = acc.astype(BF16)


def intra_kernel(q_ref, k_ref, v_ref, wq_ref, wk_ref, o_ref):
    length, width = q_ref.shape[0], wq_ref.shape[1]
    half = length // 2
    many = wq_ref.shape[0]
    cols = [slice(h * width, (h + 1) * width) for h in range(many)]
    phis = feats(
        [q_ref[:, c] for c in cols] + [k_ref[:, c] for c in cols],
        [wq_ref[h] for h in range(many)] + [wk_ref[h] for h in range(many)],
    )
    scores = [mm(phis[h].T, phis[many + h]) for h in range(many)]
    t = lax.broadcasted_iota(jnp.int32, (length, length), 0)
    s = lax.broadcasted_iota(jnp.int32, (length, length), 1)
    scores = [jnp.where(s <= t, x, 0.0) for x in scores]
    rid = lax.broadcasted_iota(jnp.int32, (EXTRA, half), 0)
    ones = jnp.ones((EXTRA, length), BF16)
    for h, score in enumerate(scores):
        to = slice(h % 2 * width, (h % 2 + 1) * width)
        num = mm(score.astype(BF16), v_ref[:, cols[h]])
        o_ref[h // 2, :length, to] = num.astype(BF16)
        fold = score[:, :half] + score[:, half:]
        hi = fold.astype(BF16)
        lo = (fold - hi.astype(F32)).astype(BF16)
        den = mm(ones, jnp.concatenate([hi, lo], axis=1), NT)
        den = jnp.where(rid < 2, den[:, :half], den[:, half:])
        dhi = den.astype(BF16).astype(F32)
        den = jnp.where(rid % 2 == 1, den - dhi, dhi)
        o_ref[h // 2, length:, to] = den.astype(BF16)


def phi_kernel(ids_ref, q_ref, w_ref, o_ref):
    i = pl.program_id(0)
    me = lax.axis_index("dp")
    width = w_ref.shape[1]
    many = o_ref.shape[1] // BLK
    pieces = q_ref.shape[1] // BLK
    xs = []
    for g in range(0, many, 4):
        rows = []
        for j in range(g, g + 4):
            b = ids_ref[i * many + j]
            rows.append(q_ref[b // pieces, pl.ds(pl.multiple_of(b % pieces * BLK, BLK), BLK), :])
        xs.append(jnp.concatenate(rows, axis=0))
    units = [(g, h) for g in range(len(xs)) for h in range(2)]
    phis = feats(
        [xs[g][:, h * width : (h + 1) * width] for g, h in units],
        [w_ref[2 * me + h] for g, h in units],
    )
    for phi, (g, h) in zip(phis, units):
        o_ref[h, 4 * g * BLK : 4 * (g + 1) * BLK, :] = phi.T


def combine_kernel(ids_ref, len_ref, sq_ref, part_ref, phi_ref, *refs):
    parts = refs[: 2 * SIDE]
    o_ref, s_ref, t_ref = refs[2 * SIDE :]
    length = part_ref.shape[1] - EXTRA
    width = part_ref.shape[2] // 2
    full = phi_ref.shape[2]
    pieces = length // BLK
    many = phi_ref.shape[1] // BLK
    i = pl.program_id(0)

    @pl.when(i == 0)
    def _():
        for h in range(2):
            acc = parts[SIDE * h][...].astype(F32)
            for d in range(1, SIDE):
                acc = acc + parts[SIDE * h + d][...].astype(F32)
            s_ref[h] = acc[:full].astype(BF16)
            row = jnp.concatenate([acc[full : full + 1], acc[full + 1 : full + 2]], axis=1)
            t_ref[h] = jnp.broadcast_to(row, t_ref.shape[1:]).astype(BF16)

    per = (o_ref.shape[1] - EXTRA) // BLK
    cut = 2 * width // 8
    col = lax.broadcasted_iota(jnp.int32, (EXTRA, 2 * width), 1)
    r = jnp.broadcast_to(sq_ref[...], col.shape)
    r1 = r.astype(BF16).astype(F32)
    r2 = (r - r1).astype(BF16).astype(F32)
    r3 = r - r1 - r2
    low = jnp.where(col < cut, r1, jnp.where(col < 2 * cut, r2, r3)).astype(BF16)
    for d in range(o_ref.shape[0]):
        o_ref[d, per * BLK :, :] = low
    nums = [mm(phi_ref[h], s_ref[h]).astype(BF16) for h in range(2)]
    dens = [mm(phi_ref[h], t_ref[h], NT).astype(BF16) for h in range(2)]
    rid = lax.broadcasted_iota(jnp.int32, (EXTRA, width), 0)
    row = lax.broadcasted_iota(jnp.int32, (BLK, 1), 0)
    for j in range(many):
        b = ids_ref[i * many + j]
        r, c = b // pieces, b % pieces
        pick = (rid // 2 == c // 2).astype(BF16)
        rows = slice(j * BLK, (j + 1) * BLK)
        for h in range(2):
            cols = slice(h * width, (h + 1) * width)
            num = part_ref[r, pl.ds(pl.multiple_of(c * BLK, BLK), BLK), cols].astype(F32)
            den = mm(part_ref[r, length:, cols], pick, TN)
            den = jnp.where(c % 2 == 0, den[:BLK], den[BLK:])
            num = nums[h][rows].astype(F32) + num
            den = dens[h][rows].astype(F32) + den
            out = jnp.where(row < len_ref[r] - c * BLK, num / den, 0.0)
            o_ref[j // per, j % per * BLK : (j % per + 1) * BLK, cols] = out.astype(BF16)


def hop(dx, dy):
    return [
        (x * SIDE + y, (x + dx) % SIDE * SIDE + (y + dy) % SIDE)
        for x in range(SIDE)
        for y in range(SIDE)
    ]


def body(
    resp_q,
    resp_k,
    resp_v,
    prompt_k,
    prompt_v,
    prompt_len,
    resp_len,
    assign,
    rewards,
    feat_q,
    feat_k,
):
    dp = lax.axis_size("dp")
    groups = lax.axis_size("group")
    heads, width, feat = feat_q.shape
    length = resp_q.shape[1]
    pieces = length // BLK
    slots = assign.shape[1]
    two = 2 * width
    tall = length + EXTRA
    q, k, v, pk, pv = resp_q[0], resp_k[0], resp_v[0], prompt_k[0], prompt_v[0]

    part = two // 8
    q_all = pl.pallas_call(
        spread_kernel,
        grid=(2,),
        in_specs=[
            pl.BlockSpec(assign.shape, lambda o: (0, 0)),
            pl.BlockSpec(resp_len.shape, lambda o: (0, 0)),
            pl.BlockSpec(rewards.shape, lambda o: (0, 0)),
            pl.BlockSpec((length, heads * width // 2), lambda o: (0, o)),
        ],
        out_specs=pl.BlockSpec((dp // 2, tall, two), lambda o: (o, 0, 0)),
        out_shape=jax.ShapeDtypeStruct((dp, tall, two), BF16),
        name="spread",
    )(assign, resp_len, rewards, q)
    q_all = lax.all_to_all(q_all, "dp", 0, 0, tiled=True)
    tabs = q_all[:, length, :].astype(F32)
    ids = tabs[:, :slots].astype(jnp.int32).reshape(-1)
    lens = tabs[:, slots].astype(jnp.int32)
    reward_all = tabs[:, part] + tabs[:, 2 * part] + tabs[:, 3 * part]

    srows = 2 * feat + EXTRA
    states = pl.pallas_call(
        state_kernel,
        grid=(SIDE,),
        in_specs=[
            pl.BlockSpec(memory_space=pltpu.SMEM),
            pl.BlockSpec(pk.shape, lambda j: (0, 0)),
            pl.BlockSpec(pv.shape, lambda j: (0, 0)),
            pl.BlockSpec(feat_k.shape, lambda j: (0, 0, 0)),
        ],
        out_specs=[pl.BlockSpec((1, srows, width), lambda j: (j, 0, 0))] * (2 * SIDE),
        out_shape=[jax.ShapeDtypeStruct((SIDE, srows, width), BF16)] * (2 * SIDE),
        name="state",
    )(prompt_len, pk, pv, feat_k)
    states = list(states)
    for p in range(2):
        for s in range(1, SIDE):
            i = SIDE * p + s
            states[i] = lax.ppermute(states[i], "dp", hop(s, 0) if p == 0 else hop(0, s))
    states = pl.pallas_call(
        add_kernel,
        in_specs=[pl.BlockSpec(memory_space=pltpu.VMEM)] * (2 * SIDE),
        out_shape=[jax.ShapeDtypeStruct((srows, width), BF16)] * (2 * SIDE),
        name="add",
    )(*states)
    states = list(states)
    for p in range(2):
        for s in range(1, SIDE):
            i = SIDE * p + s
            states[i] = lax.ppermute(states[i], "dp", hop(0, s) if p == 0 else hop(s, 0))

    inner = pl.pallas_call(
        intra_kernel,
        grid=(heads // 8,),
        in_specs=[pl.BlockSpec((length, 8 * width), lambda o: (0, o))] * 3
        + [pl.BlockSpec((8, width, feat), lambda o: (o, 0, 0))] * 2,
        out_specs=pl.BlockSpec((4, tall, two), lambda o: (o, 0, 0)),
        out_shape=jax.ShapeDtypeStruct((dp, tall, two), BF16),
        name="intra",
    )(q, k, v, feat_q, feat_k)
    inner = lax.all_to_all(inner, "dp", 0, 0, tiled=True)

    centred = reward_all - jnp.sum(reward_all) / dp
    squares = lax.ppermute(
        jnp.sum(centred * centred).reshape(1, 1),
        ("group", "dp"),
        [(g * dp + d, (g + d) % groups * dp + d) for g in range(groups) for d in range(dp)],
    )

    short = slots * BLK + EXTRA
    total = dp * slots
    many = 8
    phi = pl.pallas_call(
        phi_kernel,
        grid=(total // many,),
        in_specs=[
            pl.BlockSpec(memory_space=pltpu.SMEM),
            pl.BlockSpec((dp, tall, two), lambda i: (0, 0, 0)),
            pl.BlockSpec(feat_q.shape, lambda i: (0, 0, 0)),
        ],
        out_specs=pl.BlockSpec((2, many * BLK, 2 * feat), lambda i: (0, i, 0)),
        out_shape=jax.ShapeDtypeStruct((2, total * BLK, 2 * feat), BF16),
        name="phi",
    )(ids, q_all, feat_q)
    out = pl.pallas_call(
        combine_kernel,
        grid=(total // many,),
        in_specs=[
            pl.BlockSpec(memory_space=pltpu.SMEM),
            pl.BlockSpec(memory_space=pltpu.SMEM),
            pl.BlockSpec((1, 1), lambda i: (0, 0)),
            pl.BlockSpec((dp, tall, two), lambda i: (0, 0, 0)),
            pl.BlockSpec((2, many * BLK, 2 * feat), lambda i: (0, i, 0)),
        ]
        + [pl.BlockSpec((srows, width), lambda i: (0, 0))] * (2 * SIDE),
        out_specs=pl.BlockSpec((many // slots, short, two), lambda i: (i, 0, 0)),
        out_shape=jax.ShapeDtypeStruct((dp, short, two), BF16),
        scratch_shapes=[
            pltpu.VMEM((2, 2 * feat, width), BF16),
            pltpu.VMEM((2, width, 2 * feat), BF16),
        ],
        name="combine",
    )(ids, lens, squares, inner, phi, *states)
    out = lax.all_to_all(out, "dp", 0, 0, tiled=True)
    attn = jnp.swapaxes(out[:, : slots * BLK], 0, 1).reshape(1, slots * BLK, heads * width)

    squares = out[:, slots * BLK, :].astype(F32)
    spread = jnp.sum(squares[:, 0] + squares[:, part] + squares[:, 2 * part])
    advantage = centred / jnp.sqrt(spread / (groups * dp) + 1e-06)
    own = assign[0]
    picker = (own // pieces)[:, None] == jnp.arange(dp)[None, :]
    slot_adv = jnp.sum(jnp.where(picker, advantage[None, :], 0.0), axis=1)
    slot_len = jnp.sum(jnp.where(picker, lens[None, :], 0), axis=1)
    positions = (own % pieces)[:, None] * BLK + jnp.arange(BLK)[None, :]
    token_adv = jnp.where(positions < slot_len[:, None], slot_adv[:, None], F32(0.0))
    return (attn, token_adv.reshape(1, slots * BLK))


def solution(mesh):
    return jax.shard_map(
        body,
        mesh=mesh,
        in_specs=(
            P("group", "dp", None),
            P("group", "dp", None),
            P("group", "dp", None),
            P("group", "dp", None),
            P("group", "dp", None),
            P("group"),
            P("group", "dp"),
            P("group", "dp"),
            P("group", "dp"),
            P(),
            P(),
        ),
        out_specs=(P("group", "dp", None), P("group", "dp")),
        check_vma=False,
    )
```
